8 devices in a mesh: ep: 2 (over z, y), dp: 4 (over x, core).
Axes of the slice: x: 2, y: 2, z: 1, core: 2. Of those that a mesh axis runs over, the one named last changes fastest.
Arguments:
- tokens: bfloat16 [8192, 1536], P(('dp', 'ep'))
- d_out: bfloat16 [8192, 1536], P(('dp', 'ep'))
- expert_ids: int32 [8192, 8], P(('dp', 'ep'))
- norm_gain: bfloat16 [1536], replicated
- router: bfloat16 [1536, 40], replicated
- w_gate: bfloat16 [40, 1536, 512], P('ep')
- w_up: bfloat16 [40, 1536, 512], P('ep')
- w_down: bfloat16 [40, 512, 1536], P('ep')
Outputs:
- output 1: bfloat16 [8192, 1536], P(('dp', 'ep'))
- output 2: float32 [1], replicated
- output 3: bfloat16 [8192, 1536], P(('dp', 'ep'))
- output 4: float32 [1536, 40], replicated
- output 5: bfloat16 [40, 1536, 512], P('ep')
- output 6: bfloat16 [40, 1536, 512], P('ep')
- output 7: bfloat16 [40, 512, 1536], P('ep')
All inputs are finite; a program needn't handle non-finite values.
Results may differ from the reference program's by a relative error of at most 0.0142087.
Values are sent between devices in bfloat16 or wider.
A program may use at most 1 GiB of HBM per device.

```python
import jax
import jax.numpy as jnp
from jax import lax

TOKENS_DEV = 1024
D = 1536
FF = 512
EXPERTS = 40
TOP = 8
DEVICES = 8
CAPACITY = 416
AUX_COEF = 0.001
NORM_EPS = 1e-6
TOTAL_TOKENS = DEVICES * TOKENS_DEV
FULL_EXPERTS = max(1, (TOKENS_DEV * TOP) // (2 * CAPACITY))


def device_routing(dev_key, global_order):
    key_shift, key_pert, key_perm = jax.random.split(dev_key, 3)
    shift_pos = jax.random.randint(key_shift, (), 0, EXPERTS - 1)
    rest_pos = (shift_pos + jnp.arange(EXPERTS - 1)) % (EXPERTS - 1)
    expert_order = jnp.concatenate([global_order[:1], global_order[1:][rest_pos]])
    n_rest = EXPERTS - FULL_EXPERTS
    rest_total = TOKENS_DEV * TOP - FULL_EXPERTS * CAPACITY
    base_count = rest_total // n_rest
    extra_count = rest_total % n_rest
    rank_pos = jnp.arange(EXPERTS)
    rest_rank = jnp.maximum(rank_pos - FULL_EXPERTS, 0)
    deltas = jax.random.randint(key_pert, (EXPERTS,), 0, base_count // 2 + 1)
    pair_delta = deltas[rest_rank // 2]
    paired = ((rest_rank // 2) * 2 + 1 < n_rest).astype(jnp.int32)
    signed = jnp.where(rest_rank % 2 == 0, pair_delta, -pair_delta) * paired
    rest_count = base_count + (rest_rank < extra_count).astype(jnp.int32) + signed
    by_rank = jnp.where(rank_pos < FULL_EXPERTS, CAPACITY, rest_count)
    counts = jnp.zeros((EXPERTS,), jnp.int32).at[expert_order].set(by_rank)
    count_ends = jnp.cumsum(counts)
    sorted_ids = jnp.searchsorted(count_ends, jnp.arange(TOKENS_DEV * TOP), side="right")
    choice_grid = sorted_ids.reshape(TOP, TOKENS_DEV).T
    token_perm = jax.random.permutation(key_perm, TOKENS_DEV)
    return choice_grid[token_perm].astype(jnp.int32)


def setup_inputs(seed: int = 0) -> dict:
    key_list = jax.random.split(jax.random.key(seed), 9)
    global_order = jax.random.permutation(key_list[0], EXPERTS)
    route_keys = jax.random.split(key_list[1], DEVICES)
    expert_ids = jax.vmap(device_routing, in_axes=(0, None))(route_keys, global_order).reshape(TOTAL_TOKENS, TOP)
    router32 = jax.random.normal(key_list[2], (D, EXPERTS), jnp.float32) * D ** -0.5
    chosen = jnp.zeros((TOTAL_TOKENS, EXPERTS), jnp.float32)
    for pick_pos in range(TOP):
        chosen = chosen + (expert_ids[:, pick_pos:pick_pos + 1] == jnp.arange(EXPERTS)[None, :]).astype(jnp.float32)
    lift_rows = 1.5 * jnp.dot(chosen, router32.T)
    tokens32 = jax.random.normal(key_list[3], (TOTAL_TOKENS, D), jnp.float32) + lift_rows
    d_out32 = jax.random.normal(key_list[4], (TOTAL_TOKENS, D), jnp.float32)
    gain32 = 1.0 + 0.25 * jax.random.normal(key_list[5], (D,), jnp.float32)
    gate_w32 = jax.random.normal(key_list[6], (EXPERTS, D, FF), jnp.float32) * D ** -0.5
    up_w32 = jax.random.normal(key_list[7], (EXPERTS, D, FF), jnp.float32) * D ** -0.5
    down_w32 = jax.random.normal(key_list[8], (EXPERTS, FF, D), jnp.float32) * (0.5 * EXPERTS * TOP ** -0.5 * FF ** -0.5)
    return {
        "tokens": tokens32.astype(jnp.bfloat16),
        "d_out": d_out32.astype(jnp.bfloat16),
        "expert_ids": expert_ids,
        "norm_gain": gain32.astype(jnp.bfloat16),
        "router": router32.astype(jnp.bfloat16),
        "w_gate": gate_w32.astype(jnp.bfloat16),
        "w_up": up_w32.astype(jnp.bfloat16),
        "w_down": down_w32.astype(jnp.bfloat16),
    }


def moe_forward(tokens32, router32, gate_w32, up_w32, down_w32, norm32, expert_ids):
    inv_rms = lax.rsqrt(jnp.mean(tokens32 * tokens32, axis=1, keepdims=True) + NORM_EPS)
    normed = (tokens32 * inv_rms * norm32).astype(jnp.bfloat16)
    logits = jnp.dot(normed.astype(jnp.float32), router32)
    router_probs = jax.nn.softmax(logits, axis=1)
    gate_vals = jnp.take_along_axis(router_probs, expert_ids, axis=1)
    counts = jnp.bincount(expert_ids.reshape(-1), length=EXPERTS).astype(jnp.float32)
    aux_loss = AUX_COEF * EXPERTS * jnp.sum(counts / (TOTAL_TOKENS * TOP) * jnp.mean(router_probs, axis=0))

    def block_mix(block_in):
        rows_in, idx_blk, gate_blk = block_in
        flat_ids = idx_blk.reshape(-1)
        expert_hits = (flat_ids[:, None] == jnp.arange(EXPERTS)[None, :]).astype(jnp.int32)
        slot_rank = jnp.sum((jnp.cumsum(expert_hits, axis=0) - 1) * expert_hits, axis=1)
        dest_row = flat_ids * CAPACITY + slot_rank
        source_tok = jnp.full((EXPERTS * CAPACITY,), TOKENS_DEV, jnp.int32).at[dest_row].set(jnp.arange(TOKENS_DEV * TOP, dtype=jnp.int32) // TOP)
        packed = jnp.take(rows_in, source_tok, axis=0, mode="fill", fill_value=0).reshape(EXPERTS, CAPACITY, D).astype(jnp.float32)
        act_gate = jnp.einsum("ecd,edf->ecf", packed, gate_w32)
        act_up = jnp.einsum("ecd,edf->ecf", packed, up_w32)
        hidden = (jax.nn.silu(act_gate) * act_up).astype(jnp.bfloat16)
        result = jnp.einsum("ecf,efd->ecd", hidden.astype(jnp.float32), down_w32).astype(jnp.bfloat16)
        picked = jnp.take(result.reshape(EXPERTS * CAPACITY, D), dest_row, axis=0).reshape(TOKENS_DEV, TOP, D)
        return jnp.sum(gate_blk[:, :, None] * picked.astype(jnp.float32), axis=1)

    mixed_sum = lax.map(jax.checkpoint(block_mix), (normed.reshape(DEVICES, TOKENS_DEV, D), expert_ids.reshape(DEVICES, TOKENS_DEV, TOP), gate_vals.reshape(DEVICES, TOKENS_DEV, TOP)))
    layer_out = (tokens32 + mixed_sum.reshape(TOTAL_TOKENS, D)).astype(jnp.bfloat16)
    return layer_out, aux_loss


def reference(tokens, d_out, expert_ids, norm_gain, router, w_gate, w_up, w_down):
    norm32 = norm_gain.astype(jnp.float32)

    def loss_parts(tokens32, router32, gate_w32, up_w32, down_w32):
        return moe_forward(tokens32, router32, gate_w32, up_w32, down_w32, norm32, expert_ids)

    (layer_out, aux_loss), pullback = jax.vjp(loss_parts, tokens.astype(jnp.float32), router.astype(jnp.float32), w_gate.astype(jnp.float32), w_up.astype(jnp.float32), w_down.astype(jnp.float32))
    d_tokens, d_router, d_gate, d_up, d_down = pullback((d_out, jnp.ones_like(aux_loss)))
    return (layer_out, aux_loss.reshape(1), d_tokens.astype(jnp.bfloat16), d_router, d_gate.astype(jnp.bfloat16), d_up.astype(jnp.bfloat16), d_down.astype(jnp.bfloat16))
```

```python
import functools

import jax
import jax.numpy as jnp
from jax import lax
from jax.experimental import pallas as pl
from jax.experimental.pallas import tpu as pltpu
from jax.sharding import PartitionSpec as P

AUX_COEF = 0.001
NORM_EPS = 1e-6
MAX_HITS = 416
BLOCK = 256
GROUP = 16
TILE = 256
CHUNK = 128
MIX = 256
NT_DIMS = (((1,), (1,)), ((), ()))
TN_DIMS = (((0,), (0,)), ((), ()))
VMEM_LIMIT = 60 * 1024 * 1024


def norm_forward(tokens32, gain32):
    inv_rms = lax.rsqrt(jnp.mean(tokens32 * tokens32, axis=1, keepdims=True) + NORM_EPS)
    return inv_rms, (tokens32 * inv_rms * gain32).astype(jnp.bfloat16)


def norm_backward(tokens32, inv_rms, gain32, d_normed):
    d_scaled = d_normed * gain32
    return inv_rms * (d_scaled - tokens32 * (inv_rms * inv_rms) * jnp.mean(d_scaled * tokens32, axis=1, keepdims=True))


def dot32(left, right, dims=(((1,), (0,)), ((), ()))):
    return lax.dot_general(left, right, dims, preferred_element_type=jnp.float32)


def dispatch_kernel(scaled, n_exp, order, n_chunk, seg_len, seg_src, seg_dst, tail_at, tail_len, src, pos, gates, out, stack, blank, sems, tail_sem):
    step = pl.program_id(0)
    last = pl.num_programs(0) - 1
    slot = lax.rem(step, 2)

    def segment_copy(blk, buf, exp, grp):
        at = blk * n_exp + exp
        from_row = pl.multiple_of((seg_src[at] + grp) * GROUP, GROUP)
        to_row = pl.multiple_of((seg_dst[at] + grp) * GROUP, GROUP)
        return pltpu.make_async_copy(stack.at[buf, pl.ds(from_row, GROUP), :], out.at[pl.ds(to_row, GROUP), :], sems.at[buf])

    def each_segment(blk, buf, act):
        for exp in range(n_exp):
            @pl.loop(0, seg_len[blk * n_exp + exp])
            def _(grp):
                act(segment_copy(blk, buf, exp, grp))

    def each_tail(act):
        for exp in range(n_exp):
            @pl.loop(0, tail_len[exp])
            def _(grp):
                to_row = pl.multiple_of((tail_at[exp] + grp) * GROUP, GROUP)
                act(pltpu.make_async_copy(blank, out.at[pl.ds(to_row, GROUP), :], tail_sem))

    @pl.when(step == 0)
    def _():
        blank[...] = jnp.zeros_like(blank)
        each_tail(lambda copy: copy.start())

    @pl.when(step >= 2)
    def _():
        each_segment(step - 2, slot, lambda copy: copy.wait())

    @pl.loop(0, n_chunk[step])
    def _(chunk):
        row = lax.broadcasted_iota(jnp.int32, (CHUNK, BLOCK), 0) + chunk * CHUNK
        hit = pos[0, 0:1, :] == row
        if scaled:
            weight = jnp.where(hit, gates[0, 0:1, :], 0.0)
        for k in range(1, pos.shape[1]):
            here = pos[0, k:k + 1, :] == row
            hit = jnp.logical_or(hit, here)
            if scaled:
                weight = jnp.where(here, gates[0, k:k + 1, :], weight)
        picked = dot32(jnp.where(hit, 1.0, 0.0).astype(jnp.bfloat16), src[...])
        if scaled:
            picked = picked * jnp.sum(weight, axis=1, keepdims=True)
        stack[slot, pl.ds(pl.multiple_of(chunk * CHUNK, CHUNK), CHUNK), :] = picked.astype(jnp.bfloat16)

    each_segment(step, slot, lambda copy: copy.start())

    @pl.when(step == last)
    def _():
        each_segment(step - 1, 1 - slot, lambda copy: copy.wait())
        each_segment(step, slot, lambda copy: copy.wait())
        each_tail(lambda copy: copy.wait())


def dispatch(src, pos, gates, plan, rows, scaled):
    blocks, top_k, _ = pos.shape
    width = src.shape[1]
    n_exp = plan["tail_at"].shape[0]
    stack_rows = -(-(BLOCK * top_k + n_exp * (GROUP - 1)) // CHUNK) * CHUNK
    return pl.pallas_call(
        functools.partial(dispatch_kernel, scaled, n_exp),
        out_shape=jax.ShapeDtypeStruct((rows, width), jnp.bfloat16),
        grid_spec=pltpu.PrefetchScalarGridSpec(
            num_scalar_prefetch=7,
            grid=(blocks,),
            in_specs=[
                pl.BlockSpec((BLOCK, width), lambda i, order, *_: (order[i], 0)),
                pl.BlockSpec((1, top_k, BLOCK), lambda i, *_: (i, 0, 0)),
                pl.BlockSpec((1, top_k, BLOCK), lambda i, *_: (i, 0, 0)),
            ],
            out_specs=pl.BlockSpec(memory_space=pl.ANY),
            scratch_shapes=[
                pltpu.VMEM((2, stack_rows, width), jnp.bfloat16),
                pltpu.VMEM((GROUP, width), jnp.bfloat16),
                pltpu.SemaphoreType.DMA((2,)),
                pltpu.SemaphoreType.DMA,
            ],
        ),
        compiler_params=pltpu.CompilerParams(dimension_semantics=("arbitrary",), vmem_limit_bytes=VMEM_LIMIT),
        cost_estimate=pl.CostEstimate(flops=20_000_000_000, bytes_accessed=80_000_000, transcendentals=0),
        name="dispatch_scaled" if scaled else "dispatch",
    )(plan["order"], plan["n_chunk"], plan["seg_len"], plan["seg_src"], plan["seg_dst"], plan["tail_at"], plan["tail_len"], src, pos, gates)


def combine_kernel(weighted, n_exp, order, n_mix, seg_len, seg_src, seg_dst, rows, pos, gates, d_out, *rest):
    if weighted:
        out, d_gates, stack, sems = rest
    else:
        out, stack, sems = rest
    step = pl.program_id(0)
    last = pl.num_programs(0) - 1
    slot = lax.rem(step, 2)

    def each_segment(blk, buf, act):
        for exp in range(n_exp):
            @pl.loop(0, seg_len[blk * n_exp + exp])
            def _(grp):
                at = blk * n_exp + exp
                to_row = pl.multiple_of((seg_src[at] + grp) * GROUP, GROUP)
                from_row = pl.multiple_of((seg_dst[at] + grp) * GROUP, GROUP)
                act(pltpu.make_async_copy(rows.at[pl.ds(from_row, GROUP), :], stack.at[buf, pl.ds(to_row, GROUP), :], sems.at[buf]))

    @pl.when(step == 0)
    def _():
        @pl.loop(0, stack.shape[1] // MIX)
        def _(part):
            stack[:, pl.ds(pl.multiple_of(part * MIX, MIX), MIX), :] = jnp.zeros((2, MIX, stack.shape[2]), stack.dtype)
        each_segment(0, 0, lambda copy: copy.start())

    @pl.when(step < last)
    def _():
        each_segment(step + 1, 1 - slot, lambda copy: copy.start())

    each_segment(step, slot, lambda copy: copy.wait())
    out[...] = jnp.zeros_like(out)
    if weighted:
        d_gates[...] = jnp.zeros_like(d_gates)

    @pl.loop(0, n_mix[step])
    def _(part):
        col = lax.broadcasted_iota(jnp.int32, (BLOCK, MIX), 1) + part * MIX
        part_rows = stack[slot, pl.ds(pl.multiple_of(part * MIX, MIX), MIX), :]
        top_k = pos.shape[2]
        if weighted:
            cross = dot32(d_out[...], part_rows, NT_DIMS)
            weight = jnp.zeros((BLOCK, MIX), jnp.float32)
            d_cols = []
            for k in range(top_k):
                here = pos[0, :, k:k + 1] == col
                weight = jnp.where(here, gates[0, :, k:k + 1], weight)
                d_cols.append(jnp.sum(jnp.where(here, cross, 0.0), axis=1, keepdims=True))
            d_gates[0] += jnp.concatenate(d_cols, axis=1)
            high = weight.astype(jnp.bfloat16)
            left = weight - high.astype(jnp.float32)
            mid = left.astype(jnp.bfloat16)
            low = (left - mid.astype(jnp.float32)).astype(jnp.bfloat16)
            out[...] += dot32(high, part_rows) + dot32(mid, part_rows) + dot32(low, part_rows)
        else:
            hit = pos[0, :, 0:1] == col
            for k in range(1, top_k):
                hit = jnp.logical_or(hit, pos[0, :, k:k + 1] == col)
            out[...] += dot32(jnp.where(hit, 1.0, 0.0).astype(jnp.bfloat16), part_rows)


def combine(rows, pos_t, gates_t, d_out, plan, weighted):
    blocks, _, top_k = pos_t.shape
    width = rows.shape[1]
    n_exp = plan["tail_at"].shape[0]
    stack_rows = -(-(BLOCK * top_k + n_exp * (GROUP - 1)) // MIX) * MIX
    out_shape = [jax.ShapeDtypeStruct((blocks * BLOCK, width), jnp.float32)]
    out_specs = [pl.BlockSpec((BLOCK, width), lambda i, *_: (i, 0))]
    if weighted:
        out_shape.append(jax.ShapeDtypeStruct((blocks, BLOCK, top_k), jnp.float32))
        out_specs.append(pl.BlockSpec((1, BLOCK, top_k), lambda i, *_: (i, 0, 0)))
    d_spec = pl.BlockSpec((BLOCK, width), lambda i, order, *_: (order[i], 0)) if weighted else pl.BlockSpec((GROUP, width), lambda i, *_: (0, 0))
    return pl.pallas_call(
        functools.partial(combine_kernel, weighted, n_exp),
        out_shape=out_shape,
        grid_spec=pltpu.PrefetchScalarGridSpec(
            num_scalar_prefetch=5,
            grid=(blocks,),
            in_specs=[
                pl.BlockSpec(memory_space=pl.ANY),
                pl.BlockSpec((1, BLOCK, top_k), lambda i, *_: (i, 0, 0)),
                pl.BlockSpec((1, BLOCK, top_k), lambda i, *_: (i, 0, 0)),
                d_spec,
            ],
            out_specs=out_specs,
            scratch_shapes=[
                pltpu.VMEM((2, stack_rows, width), jnp.bfloat16),
                pltpu.SemaphoreType.DMA((2,)),
            ],
        ),
        compiler_params=pltpu.CompilerParams(dimension_semantics=("arbitrary",), vmem_limit_bytes=VMEM_LIMIT),
        cost_estimate=pl.CostEstimate(flops=30_000_000_000 if weighted else 10_000_000_000, bytes_accessed=60_000_000, transcendentals=0),
        name="combine_weighted" if weighted else "combine",
    )(plan["order"], plan["n_mix"], plan["seg_len"], plan["seg_src"], plan["seg_dst"], rows, pos_t, gates_t, d_out)


def forward_kernel(tile_exp, tile_at, own_at, tile_kind, x, w_gate, w_up, w_down, act_gate, act_up, hidden, result):
    kind = tile_kind[pl.program_id(0)]

    @pl.when(kind > 0)
    def _():
        a = dot32(x[...], w_gate[0])
        b = dot32(x[...], w_up[0])
        u = (a * jax.nn.sigmoid(a) * b).astype(jnp.bfloat16)
        act_gate[...] = a
        act_up[...] = b
        hidden[...] = u

    @pl.when(kind > 1)
    def _():
        result[...] = dot32(hidden[...], w_down[0]).astype(jnp.bfloat16)


def inward_kernel(tile_exp, tile_at, own_at, tile_kind, d_rows, act_gate, act_up, w_gate, w_up, w_down, d_gate, d_up, d_in):
    kind = tile_kind[pl.program_id(0)]

    @pl.when(kind > 0)
    def _():
        d_hidden = dot32(d_rows[...], w_down[0], NT_DIMS)
        a = act_gate[...]
        sig = jax.nn.sigmoid(a)
        d_gate[...] = (d_hidden * act_up[...] * sig * (1.0 + a * (1.0 - sig))).astype(jnp.bfloat16)
        d_up[...] = (d_hidden * (a * sig)).astype(jnp.bfloat16)

    @pl.when(kind > 1)
    def _():
        d_in[...] = (dot32(d_gate[...], w_gate[0], NT_DIMS) + dot32(d_up[...], w_up[0], NT_DIMS)).astype(jnp.bfloat16)


def grads_kernel(pair_tile, pair_next, pair_exp, pair_kind, pair_first, pair_last, x0, x1, a0, a1, b0, b1, u0, u1, d0, d1, g_gate, g_up, g_down, s_gate, s_up, s_down):
    step = pl.program_id(0)

    @pl.when(pair_first[step] > 0)
    def _():
        s_gate[...] = jnp.zeros_like(s_gate)
        s_up[...] = jnp.zeros_like(s_up)
        s_down[...] = jnp.zeros_like(s_down)

    def add(total, left, right):
        total[...] += dot32(left, right, TN_DIMS)

    @pl.when(pair_kind[step] > 1)
    def _():
        x = jnp.concatenate([x0[...], x1[...]], axis=0)
        d = jnp.concatenate([d0[...], d1[...]], axis=0)
        add(s_gate, x, jnp.concatenate([a0[...], a1[...]], axis=0))
        add(s_up, x, jnp.concatenate([b0[...], b1[...]], axis=0))
        add(s_down, jnp.concatenate([u0[...], u1[...]], axis=0), d)

    @pl.when(pair_kind[step] == 1)
    def _():
        add(s_gate, x0[...], a0[...])
        add(s_up, x0[...], b0[...])
        add(s_down, u0[...], d0[...])

    @pl.when(pair_last[step] > 0)
    def _():
        g_gate[0] = s_gate[...].astype(jnp.bfloat16)
        g_up[0] = s_up[...].astype(jnp.bfloat16)
        g_down[0] = s_down[...].astype(jnp.bfloat16)


def tile_specs(width, mid):
    wide = pl.BlockSpec((TILE, width), lambda t, exp, at, own, kind: (at[t], 0))
    thin = pl.BlockSpec((TILE, mid), lambda t, exp, at, own, kind: (at[t], 0))
    owned = pl.BlockSpec((TILE, width), lambda t, exp, at, own, kind: (own[t], 0))
    w_in = pl.BlockSpec((1, width, mid), lambda t, exp, at, own, kind: (exp[t], 0, 0))
    w_out = pl.BlockSpec((1, mid, width), lambda t, exp, at, own, kind: (exp[t], 0, 0))
    return wide, thin, owned, w_in, w_out


def forward_tiles(x, w_gate, w_up, w_down, plan):
    rows, width = x.shape
    mid = w_gate.shape[2]
    max_tiles = rows // TILE
    wide, thin, owned, w_in, w_out = tile_specs(width, mid)
    return pl.pallas_call(
        forward_kernel,
        out_shape=[
            jax.ShapeDtypeStruct((rows, mid), jnp.float32),
            jax.ShapeDtypeStruct((rows, mid), jnp.float32),
            jax.ShapeDtypeStruct((rows, mid), jnp.bfloat16),
            jax.ShapeDtypeStruct((rows, width), jnp.bfloat16),
        ],
        grid_spec=pltpu.PrefetchScalarGridSpec(
            num_scalar_prefetch=4,
            grid=(max_tiles,),
            in_specs=[wide, w_in, w_in, w_out],
            out_specs=[thin, thin, thin, owned],
        ),
        compiler_params=pltpu.CompilerParams(dimension_semantics=("arbitrary",), vmem_limit_bytes=VMEM_LIMIT),
        cost_estimate=pl.CostEstimate(flops=70_000_000_000, bytes_accessed=250_000_000, transcendentals=0),
        name="forward_tiles",
    )(plan["tile_exp"], plan["tile_at"], plan["own_at"], plan["tile_kind"], x, w_gate, w_up, w_down)


def inward_tiles(d_rows, act_gate, act_up, w_gate, w_up, w_down, plan):
    rows, width = d_rows.shape
    mid = w_gate.shape[2]
    max_tiles = rows // TILE
    wide, thin, owned, w_in, w_out = tile_specs(width, mid)
    return pl.pallas_call(
        inward_kernel,
        out_shape=[
            jax.ShapeDtypeStruct((rows, mid), jnp.bfloat16),
            jax.ShapeDtypeStruct((rows, mid), jnp.bfloat16),
            jax.ShapeDtypeStruct((rows, width), jnp.bfloat16),
        ],
        grid_spec=pltpu.PrefetchScalarGridSpec(
            num_scalar_prefetch=4,
            grid=(max_tiles,),
            in_specs=[wide, thin, thin, w_in, w_in, w_out],
            out_specs=[thin, thin, owned],
        ),
        compiler_params=pltpu.CompilerParams(dimension_semantics=("arbitrary",), vmem_limit_bytes=VMEM_LIMIT),
        cost_estimate=pl.CostEstimate(flops=60_000_000_000, bytes_accessed=250_000_000, transcendentals=0),
        name="inward_tiles",
    )(plan["tile_exp"], plan["tile_at"], plan["own_at"], plan["tile_kind"], d_rows, act_gate, act_up, w_gate, w_up, w_down)


def grad_tiles(x, d_gate, d_up, hidden, d_rows, plan):
    rows, width = x.shape
    mid = d_gate.shape[1]
    n_exp = plan["tail_at"].shape[0]
    wide0 = pl.BlockSpec((TILE, width), lambda s, tile, *_: (tile[s], 0))
    thin0 = pl.BlockSpec((TILE, mid), lambda s, tile, *_: (tile[s], 0))
    wide1 = pl.BlockSpec((TILE, width), lambda s, tile, after, *_: (after[s], 0))
    thin1 = pl.BlockSpec((TILE, mid), lambda s, tile, after, *_: (after[s], 0))
    g_in = pl.BlockSpec((1, width, mid), lambda s, tile, after, exp, *_: (exp[s], 0, 0))
    g_out = pl.BlockSpec((1, mid, width), lambda s, tile, after, exp, *_: (exp[s], 0, 0))
    return pl.pallas_call(
        grads_kernel,
        out_shape=[
            jax.ShapeDtypeStruct((n_exp, width, mid), jnp.bfloat16),
            jax.ShapeDtypeStruct((n_exp, width, mid), jnp.bfloat16),
            jax.ShapeDtypeStruct((n_exp, mid, width), jnp.bfloat16),
        ],
        grid_spec=pltpu.PrefetchScalarGridSpec(
            num_scalar_prefetch=6,
            grid=(plan["pair_tile"].shape[0],),
            in_specs=[wide0, wide1, thin0, thin1, thin0, thin1, thin0, thin1, wide0, wide1],
            out_specs=[g_in, g_in, g_out],
            scratch_shapes=[
                pltpu.VMEM((width, mid), jnp.float32),
                pltpu.VMEM((width, mid), jnp.float32),
                pltpu.VMEM((mid, width), jnp.float32),
            ],
        ),
        compiler_params=pltpu.CompilerParams(dimension_semantics=("arbitrary",), vmem_limit_bytes=VMEM_LIMIT),
        cost_estimate=pl.CostEstimate(flops=85_000_000_000, bytes_accessed=250_000_000, transcendentals=0),
        name="grad_tiles",
    )(plan["pair_tile"], plan["pair_next"], plan["pair_exp"], plan["pair_kind"], plan["pair_first"], plan["pair_last"], x, x, d_gate, d_gate, d_up, d_up, hidden, hidden, d_rows, d_rows)


def exclusive(values, axis=0):
    return jnp.cumsum(values, axis=axis) - values


def make_plan(local_ids, order, own_blocks, n_exp, max_tiles):
    blocks = local_ids.shape[0]
    onehot = (local_ids[:, :, None, :] == jnp.arange(n_exp)[None, None, :, None]).astype(jnp.float32)
    hits = jnp.sum(onehot, axis=1)
    before = jnp.triu(jnp.ones((BLOCK, BLOCK), jnp.bfloat16), 1)
    rank = jnp.einsum("oet,ts->oes", hits.astype(jnp.bfloat16), before, preferred_element_type=jnp.float32)
    seg_len = (jnp.sum(hits, axis=2).astype(jnp.int32) + GROUP - 1) // GROUP
    seg_src = exclusive(seg_len, 1)
    per_tile = TILE // GROUP
    groups = jnp.sum(seg_len, axis=0)
    tiles = (groups + per_tile - 1) // per_tile
    tile_base = exclusive(tiles)
    seg_dst = tile_base[None, :] * per_tile + exclusive(seg_len, 0)
    place = rank + (seg_src * GROUP).astype(jnp.float32)[:, :, None]
    pos = jnp.sum(onehot * (place[:, None] + 1.0), axis=2).astype(jnp.int32) - 1
    own_tiles = (jnp.sum(seg_len[:own_blocks], axis=0) + per_tile - 1) // per_tile
    tile_ids = jnp.arange(max_tiles)
    tile_at = jnp.minimum(tile_ids, jnp.sum(tiles) - 1)
    tile_exp = jnp.sum((tile_at[:, None] >= (tile_base + tiles)[None, :]).astype(jnp.int32), axis=1)
    own_at = jnp.minimum(tile_at, (tile_base + own_tiles)[tile_exp] - 1)
    is_own = own_at == tile_at
    pairs = (tiles + 1) // 2
    pair_base = exclusive(pairs)
    pair_ids = jnp.arange(n_exp * ((max_tiles // n_exp + 1) // 2))
    pair_at = jnp.minimum(pair_ids, jnp.sum(pairs) - 1)
    pair_live = pair_ids == pair_at
    pair_exp = jnp.sum((pair_at[:, None] >= (pair_base + pairs)[None, :]).astype(jnp.int32), axis=1)
    nth = pair_at - pair_base[pair_exp]
    pair_tile = tile_base[pair_exp] + 2 * nth
    is_pair = 2 * nth + 1 < tiles[pair_exp]
    stack_rows = jnp.sum(seg_len, axis=1) * GROUP
    plan = {
        "order": order,
        "n_chunk": (stack_rows + CHUNK - 1) // CHUNK,
        "n_mix": (stack_rows + MIX - 1) // MIX,
        "seg_len": seg_len.reshape(-1),
        "seg_src": seg_src.reshape(-1),
        "seg_dst": seg_dst.reshape(-1),
        "tail_at": tile_base * per_tile + groups,
        "tail_len": tiles * per_tile - groups,
        "tile_exp": tile_exp,
        "tile_at": tile_at,
        "own_at": own_at,
        "tile_kind": jnp.where(tile_ids == tile_at, jnp.where(is_own, 2, 1), 0),
        "pair_tile": pair_tile,
        "pair_next": pair_tile + is_pair,
        "pair_exp": pair_exp,
        "pair_kind": jnp.where(pair_live, jnp.where(is_pair, 2, 1), 0),
        "pair_first": pair_live & (nth == 0),
        "pair_last": pair_live & (nth == pairs[pair_exp] - 1),
    }
    return jax.tree.map(lambda value: value.astype(jnp.int32), plan), pos


def solution(mesh):
    ep_size = mesh.shape["ep"]
    dp_size = mesh.shape["dp"]
    devices = ep_size * dp_size
    cores = 2
    tok_spec = P(("dp", "ep"), None)
    exp_spec = P("ep", None, None)
    core_perm = [(i, i ^ 1) for i in range(dp_size)]
    ep_perm = [(i, i ^ 1) for i in range(ep_size)]
    core_groups = [[i, i + 1] for i in range(0, dp_size, cores)]

    def to_owner(parts):
        half = parts.shape[0] // 2
        mine = parts[half:] + lax.ppermute(parts[:half], "dp", core_perm)
        quarter = half // 2
        return mine[quarter:] + lax.ppermute(mine[:quarter], "ep", ep_perm)

    def device_step(tokens, d_out, expert_ids, norm_gain, router, w_gate, w_up, w_down):
        tok_rows, model_width = tokens.shape
        top_k = expert_ids.shape[1]
        local_experts = w_gate.shape[0]
        experts = local_experts * ep_size
        total_tok = tok_rows * devices
        n_exp = local_experts // cores
        dev_blocks = tok_rows // BLOCK
        own_devs = devices // 2
        own_blocks = own_devs * dev_blocks
        seg_pad = devices * dev_blocks * (GROUP - 1)
        max_tiles = n_exp * -(-(devices * MAX_HITS + seg_pad) // TILE)

        ep_at = lax.axis_index("ep")
        dp_at = lax.axis_index("dp")
        core_at = lax.rem(dp_at, cores)
        x_at = lax.div(dp_at, cores)

        def dev_of(x, core, ep):
            return (x * cores + core) * ep_size + ep

        dev_order = jnp.stack(
            [dev_of(x_at, 1 - core_at, 1 - ep_at), dev_of(x_at, 1 - core_at, ep_at), dev_of(x_at, core_at, 1 - ep_at), dev_of(x_at, core_at, ep_at)]
            + [dev_of(1 - x_at, core, ep) for core in range(cores) for ep in range(ep_size)]
        )
        order = (dev_order[:, None] * dev_blocks + jnp.arange(dev_blocks)[None, :]).reshape(-1).astype(jnp.int32)

        tokens32 = tokens.astype(jnp.float32)
        gain32 = norm_gain.astype(jnp.float32)
        inv_rms, normed = norm_forward(tokens32, gain32)
        logits = jnp.dot(normed, router, preferred_element_type=jnp.float32)
        router_probs = jax.nn.softmax(logits, axis=1)
        expert_hits = expert_ids[:, :, None] == jnp.arange(experts)[None, None, :]
        gate_vals = jnp.sum(jnp.where(expert_hits, router_probs[:, None, :], 0.0), axis=2)

        prob_sums = jnp.pad(jnp.sum(router_probs, axis=0), (0, tok_rows - experts))
        packet = jnp.concatenate([expert_ids.astype(jnp.float32).T, gate_vals.T, prob_sums[None]], axis=0)
        packets = lax.all_gather(packet, ("dp", "ep"))
        all_normed = lax.all_gather(normed, ("dp", "ep"), tiled=True)
        d_out_late, _ = lax.optimization_barrier((d_out, all_normed[:8]))
        all_d_out = lax.all_gather(d_out_late, ("dp", "ep"), tiled=True)

        all_ids = packets[:, :top_k].astype(jnp.int32)
        counts = jnp.sum((all_ids[..., None] == jnp.arange(experts)).astype(jnp.float32), axis=(0, 1, 2))
        expert_frac = counts / (total_tok * top_k)
        aux_loss = AUX_COEF * experts * jnp.sum(expert_frac * jnp.sum(packets[:, 2 * top_k, :experts], axis=0)) / total_tok

        turned = jnp.take(packets, dev_order, axis=0)

        def by_block(rows):
            return rows.reshape(devices, top_k, dev_blocks, BLOCK).transpose(0, 2, 1, 3).reshape(devices * dev_blocks, top_k, BLOCK)

        first_expert = ep_at * local_experts + core_at * n_exp
        block_ids = by_block(turned[:, :top_k]).astype(jnp.int32) - first_expert
        block_ids = jnp.where((block_ids >= 0) & (block_ids < n_exp), block_ids, n_exp)
        block_gates = by_block(turned[:, top_k:2 * top_k])
        plan, pos = make_plan(block_ids, order, own_blocks, n_exp, max_tiles)
        plan["tile_exp"] = plan["tile_exp"] + core_at * n_exp
        pos_t = pos[:own_blocks].transpose(0, 2, 1)
        gates_t = block_gates[:own_blocks].transpose(0, 2, 1)

        rows = max_tiles * TILE
        x = dispatch(all_normed, pos, block_gates, plan, rows, False)
        act_gate, act_up, hidden, result = forward_tiles(x, w_gate, w_up, w_down, plan)
        d_rows = dispatch(all_d_out, pos, block_gates, plan, rows, True)
        mixed_parts, d_gate_parts = combine(result, pos_t, gates_t, all_d_out, plan, True)
        d_act_gate, d_act_up, d_expert_in = inward_tiles(d_rows, act_gate, act_up, w_gate, w_up, w_down, plan)
        (d_normed_parts,) = combine(d_expert_in, pos_t, gates_t, all_d_out, plan, False)
        grad_gate, grad_up, grad_down = grad_tiles(x, d_act_gate, d_act_up, hidden, d_rows, plan)

        def both_cores(grad):
            return lax.all_gather(grad, "dp", axis_index_groups=core_groups, tiled=True)

        layer_out = (tokens32 + to_owner(mixed_parts)).astype(jnp.bfloat16)
        d_gates = to_owner(d_gate_parts).reshape(tok_rows, top_k)
        d_probs = jnp.sum(jnp.where(expert_hits, d_gates[:, :, None], 0.0), axis=1) + (AUX_COEF * experts / total_tok) * expert_frac[None, :]
        d_logits = (router_probs * (d_probs - jnp.sum(router_probs * d_probs, axis=1, keepdims=True))).astype(jnp.bfloat16)
        grad_router = lax.psum(lax.dot_general(normed, d_logits, TN_DIMS, preferred_element_type=jnp.float32), ("ep", "dp"))
        d_normed = to_owner(d_normed_parts) + lax.dot_general(d_logits, router, NT_DIMS, preferred_element_type=jnp.float32)
        d_tokens = (d_out.astype(jnp.float32) + norm_backward(tokens32, inv_rms, gain32, d_normed)).astype(jnp.bfloat16)
        return layer_out, aux_loss.reshape(1), d_tokens, grad_router, both_cores(grad_gate), both_cores(grad_up), both_cores(grad_down)

    return jax.shard_map(device_step, mesh=mesh, in_specs=(tok_spec, tok_spec, tok_spec, P(None), P(None, None), exp_spec, exp_spec, exp_spec), out_specs=(tok_spec, P(None), tok_spec, P(None, None), exp_spec, exp_spec, exp_spec), check_vma=False)
```

```python
import functools

import jax
import jax.numpy as jnp
from jax import lax
from jax.experimental import pallas as pl
from jax.experimental.pallas import tpu as pltpu
from jax.sharding import PartitionSpec as P


AUX_COEF = 0.001
NORM_EPS = 1e-6
MAX_HITS = 416
BLOCK = 256
GROUP = 16
TILE = 512
HALF = TILE // 2
CHUNK = 256
MIX = 256
NT_DIMS = (((1,), (1,)), ((), ()))
TN_DIMS = (((0,), (0,)), ((), ()))
VMEM_LIMIT = 60 * 1024 * 1024


def norm_forward(tokens32, gain32):
    inv_rms = lax.rsqrt(jnp.mean(tokens32 * tokens32, axis=1, keepdims=True) + NORM_EPS)
    return inv_rms, (tokens32 * inv_rms * gain32).astype(jnp.bfloat16)


def norm_backward(tokens32, inv_rms, gain32, d_normed):
    d_scaled = d_normed * gain32
    return inv_rms * (d_scaled - tokens32 * (inv_rms * inv_rms) * jnp.mean(d_scaled * tokens32, axis=1, keepdims=True))


def dot32(left, right, dims=(((1,), (0,)), ((), ()))):
    return lax.dot_general(left, right, dims, preferred_element_type=jnp.float32)


def dispatch_kernel(scaled, n_exp, order, n_chunk, seg_len, seg_src, seg_dst, tail_at, tail_len, src, pos, gates, out, stack, blank, sems, tail_sem):
    step = pl.program_id(0)
    last = pl.num_programs(0) - 1
    slot = lax.rem(step, 2)

    def segment_copy(blk, buf, exp, grp):
        at = blk * n_exp + exp
        from_row = pl.multiple_of((seg_src[at] + grp) * GROUP, GROUP)
        to_row = pl.multiple_of((seg_dst[at] + grp) * GROUP, GROUP)
        return pltpu.make_async_copy(stack.at[buf, pl.ds(from_row, GROUP), :], out.at[pl.ds(to_row, GROUP), :], sems.at[buf])

    def each_segment(blk, buf, act):
        for exp in range(n_exp):
            @pl.loop(0, seg_len[blk * n_exp + exp])
            def _(grp):
                act(segment_copy(blk, buf, exp, grp))

    def each_tail(act):
        for exp in range(n_exp):
            @pl.loop(0, tail_len[exp])
            def _(grp):
                to_row = pl.multiple_of((tail_at[exp] + grp) * GROUP, GROUP)
                act(pltpu.make_async_copy(blank, out.at[pl.ds(to_row, GROUP), :], tail_sem))

    @pl.when(step == 0)
    def _():
        blank[...] = jnp.zeros_like(blank)
        each_tail(lambda copy: copy.start())

    @pl.when(step >= 2)
    def _():
        each_segment(step - 2, slot, lambda copy: copy.wait())

    @pl.loop(0, n_chunk[step])
    def _(chunk):
        row = lax.broadcasted_iota(jnp.int32, (CHUNK, BLOCK), 0) + chunk * CHUNK
        hit = pos[0, 0:1, :] == row
        if scaled:
            weight = jnp.where(hit, gates[0, 0:1, :], 0.0)
        for k in range(1, pos.shape[1]):
            here = pos[0, k:k + 1, :] == row
            hit = jnp.logical_or(hit, here)
            if scaled:
                weight = jnp.where(here, gates[0, k:k + 1, :], weight)
        picked = dot32(jnp.where(hit, 1.0, 0.0).astype(jnp.bfloat16), src[...])
        if scaled:
            picked = picked * jnp.sum(weight, axis=1, keepdims=True)
        stack[slot, pl.ds(pl.multiple_of(chunk * CHUNK, CHUNK), CHUNK), :] = picked.astype(jnp.bfloat16)

    each_segment(step, slot, lambda copy: copy.start())

    @pl.when(step == last)
    def _():
        each_segment(step - 1, 1 - slot, lambda copy: copy.wait())
        each_segment(step, slot, lambda copy: copy.wait())
        each_tail(lambda copy: copy.wait())


def dispatch(src, pos, gates, plan, rows, scaled):
    blocks, top_k, _ = pos.shape
    width = src.shape[1]
    n_exp = plan["tail_at"].shape[0]
    stack_rows = -(-(BLOCK * top_k + n_exp * (GROUP - 1)) // CHUNK) * CHUNK
    return pl.pallas_call(
        functools.partial(dispatch_kernel, scaled, n_exp),
        out_shape=jax.ShapeDtypeStruct((rows, width), jnp.bfloat16),
        grid_spec=pltpu.PrefetchScalarGridSpec(
            num_scalar_prefetch=7,
            grid=(blocks,),
            in_specs=[
                pl.BlockSpec((BLOCK, width), lambda i, order, *_: (order[i], 0)),
                pl.BlockSpec((1, top_k, BLOCK), lambda i, *_: (i, 0, 0)),
                pl.BlockSpec((1, top_k, BLOCK), lambda i, *_: (i, 0, 0)),
            ],
            out_specs=pl.BlockSpec(memory_space=pl.ANY),
            scratch_shapes=[
                pltpu.VMEM((2, stack_rows, width), jnp.bfloat16),
                pltpu.VMEM((GROUP, width), jnp.bfloat16),
                pltpu.SemaphoreType.DMA((2,)),
                pltpu.SemaphoreType.DMA,
            ],
        ),
        compiler_params=pltpu.CompilerParams(dimension_semantics=("arbitrary",), vmem_limit_bytes=VMEM_LIMIT),
        cost_estimate=pl.CostEstimate(flops=20_000_000_000, bytes_accessed=80_000_000, transcendentals=0),
        name="dispatch_scaled" if scaled else "dispatch",
    )(plan["order"], plan["n_chunk"], plan["seg_len"], plan["seg_src"], plan["seg_dst"], plan["tail_at"], plan["tail_len"], src, pos, gates)


def combine_kernel(weighted, n_exp, order, n_mix, seg_len, seg_src, seg_dst, rows, pos, gates, d_out, *rest):
    if weighted:
        away, far, near, d_gates, stack, total, sems = rest
    else:
        away, far, near, stack, total, sems = rest
    step = pl.program_id(0)
    blocks = pl.num_programs(0)
    slot = lax.rem(step, 2)

    def each_segment(blk, buf, act):
        for exp in range(n_exp):
            @pl.loop(0, seg_len[blk * n_exp + exp])
            def _(grp):
                at = blk * n_exp + exp
                to_row = pl.multiple_of((seg_src[at] + grp) * GROUP, GROUP)
                from_row = pl.multiple_of((seg_dst[at] + grp) * GROUP, GROUP)
                act(pltpu.make_async_copy(rows.at[pl.ds(from_row, GROUP), :], stack.at[buf, pl.ds(to_row, GROUP), :], sems.at[buf]))

    @pl.when(step == 0)
    def _():
        @pl.loop(0, stack.shape[1] // MIX)
        def _(part):
            stack[:, pl.ds(pl.multiple_of(part * MIX, MIX), MIX), :] = jnp.zeros((2, MIX, stack.shape[2]), stack.dtype)

        each_segment(0, 0, lambda copy: copy.start())

    @pl.when(step < blocks - 1)
    def _():
        each_segment(step + 1, 1 - slot, lambda copy: copy.start())

    each_segment(step, slot, lambda copy: copy.wait())
    total[...] = jnp.zeros_like(total)
    if weighted:
        d_gates[...] = jnp.zeros_like(d_gates)

    @pl.loop(0, n_mix[step])
    def _(part):
        col = lax.broadcasted_iota(jnp.int32, (BLOCK, MIX), 1) + part * MIX
        part_rows = stack[slot, pl.ds(pl.multiple_of(part * MIX, MIX), MIX), :]
        top_k = pos.shape[2]
        if weighted:
            cross = dot32(d_out[...], part_rows, NT_DIMS)
            weight = jnp.zeros((BLOCK, MIX), jnp.float32)
            d_cols = []
            for k in range(top_k):
                here = pos[0, :, k:k + 1] == col
                weight = jnp.where(here, gates[0, :, k:k + 1], weight)
                d_cols.append(jnp.sum(jnp.where(here, cross, 0.0), axis=1, keepdims=True))
            d_gates[0] += jnp.concatenate(d_cols, axis=1)
            high = weight.astype(jnp.bfloat16)
            left = weight - high.astype(jnp.float32)
            mid = left.astype(jnp.bfloat16)
            low = (left - mid.astype(jnp.float32)).astype(jnp.bfloat16)
            mixed = dot32(jnp.concatenate([high, mid, low], axis=0), part_rows)
            total[...] += mixed[:BLOCK] + mixed[BLOCK:2 * BLOCK] + mixed[2 * BLOCK:]
        else:
            hit = pos[0, :, 0:1] == col
            for k in range(1, top_k):
                hit = jnp.logical_or(hit, pos[0, :, k:k + 1] == col)
            total[...] += dot32(jnp.where(hit, 1.0, 0.0).astype(jnp.bfloat16), part_rows)

    half, quarter = blocks // 2, blocks // 4

    @pl.when(step < half)
    def _():
        away[...] = total[...]

    @pl.when((step >= half) & (step < half + quarter))
    def _():
        far[...] = total[...]

    @pl.when(step >= half + quarter)
    def _():
        near[...] = total[...]


def combine(rows, pos_t, gates_t, d_out, plan, weighted):
    blocks, _, top_k = pos_t.shape
    width = rows.shape[1]
    n_exp = plan["tail_at"].shape[0]
    stack_rows = -(-(BLOCK * top_k + n_exp * (GROUP - 1)) // MIX) * MIX
    half, quarter = blocks // 2, blocks // 4
    out_shape, out_specs = [], []
    for first, count in ((0, half), (half, quarter), (half + quarter, quarter)):
        out_shape.append(jax.ShapeDtypeStruct((count * BLOCK, width), jnp.float32))
        out_specs.append(pl.BlockSpec((BLOCK, width), lambda i, *_, first=first, count=count: (jnp.clip(i - first, 0, count - 1), 0)))
    if weighted:
        out_shape.append(jax.ShapeDtypeStruct((blocks, BLOCK, top_k), jnp.float32))
        out_specs.append(pl.BlockSpec((1, BLOCK, top_k), lambda i, *_: (i, 0, 0)))
    d_spec = pl.BlockSpec((BLOCK, width), lambda i, order, *_: (order[i], 0)) if weighted else pl.BlockSpec((GROUP, width), lambda i, *_: (0, 0))
    return pl.pallas_call(
        functools.partial(combine_kernel, weighted, n_exp),
        out_shape=out_shape,
        grid_spec=pltpu.PrefetchScalarGridSpec(
            num_scalar_prefetch=5,
            grid=(blocks,),
            in_specs=[
                pl.BlockSpec(memory_space=pl.ANY),
                pl.BlockSpec((1, BLOCK, top_k), lambda i, *_: (i, 0, 0)),
                pl.BlockSpec((1, BLOCK, top_k), lambda i, *_: (i, 0, 0)),
                d_spec,
            ],
            out_specs=out_specs,
            scratch_shapes=[
                pltpu.VMEM((2, stack_rows, width), jnp.bfloat16),
                pltpu.VMEM((BLOCK, width), jnp.float32),
                pltpu.SemaphoreType.DMA((2,)),
            ],
        ),
        compiler_params=pltpu.CompilerParams(dimension_semantics=("arbitrary",), vmem_limit_bytes=VMEM_LIMIT),
        cost_estimate=pl.CostEstimate(flops=70_000_000_000 if weighted else 40_000_000_000, bytes_accessed=60_000_000, transcendentals=0),
        name="combine_weighted" if weighted else "combine",
    )(plan["order"], plan["n_mix"], plan["seg_len"], plan["seg_src"], plan["seg_dst"], rows, pos_t, gates_t, d_out)


def by_kind(kind, body):
    for code, rows in ((1, HALF), (2, TILE)):
        @pl.when(kind == code)
        def _():
            body(pl.ds(0, rows))


def forward_kernel(tile_exp, tile_at, own_at, tile_kind, own_kind, x, w_gate, w_up, w_down, act_gate, act_up, hidden, result):
    step = pl.program_id(0)

    def first(part):
        a = dot32(x[part], w_gate[0])
        b = dot32(x[part], w_up[0])
        act_gate[part] = a
        act_up[part] = b
        hidden[part] = (a * jax.nn.sigmoid(a) * b).astype(jnp.bfloat16)

    def second(part):
        result[part] = dot32(hidden[part], w_down[0]).astype(jnp.bfloat16)

    by_kind(tile_kind[step], first)
    by_kind(own_kind[step], second)


def inward_kernel(own, tile_exp, tile_at, tile_kind, d_rows, act_gate, act_up, *rest):
    if own:
        w_gate, w_up, w_down, d_gate, d_up, d_in = rest
    else:
        w_down, _, _, d_gate, d_up = rest

    def body(part):
        d_hidden = dot32(d_rows[part], w_down[0], NT_DIMS)
        a = act_gate[part]
        sig = jax.nn.sigmoid(a)
        d_a = (d_hidden * act_up[part] * sig * (1.0 + a * (1.0 - sig))).astype(jnp.bfloat16)
        d_b = (d_hidden * (a * sig)).astype(jnp.bfloat16)
        d_gate[part] = d_a
        d_up[part] = d_b
        if own:
            d_in[part] = (dot32(d_a, w_gate[0], NT_DIMS) + dot32(d_b, w_up[0], NT_DIMS)).astype(jnp.bfloat16)

    by_kind(tile_kind[pl.program_id(0)], body)


def grads_kernel(lefts, tile_exp, tile_at, tile_kind, tile_first, tile_last, base, *refs):
    n = len(lefts)
    left_refs, right_refs = refs[:max(lefts) + 1], refs[max(lefts) + 1:max(lefts) + 1 + n]
    outs, wholes, totals = refs[-3 * n:-2 * n], refs[-2 * n:-n], refs[-n:]
    step = pl.program_id(0)

    @pl.when(tile_first[step] > 0)
    def _():
        for total in totals:
            total[...] = jnp.zeros_like(total)

    def body(part):
        for which, right, total in zip(lefts, right_refs, totals):
            total[...] += dot32(left_refs[which][part], right[part], TN_DIMS)

    by_kind(tile_kind[step], body)

    @pl.when(tile_last[step] > 0)
    def _():
        for out, whole, total in zip(outs, wholes, totals):
            rounded = total[...].astype(jnp.bfloat16)
            out[0] = rounded
            whole[0] = rounded


def kernel_params():
    return pltpu.CompilerParams(dimension_semantics=("arbitrary",), vmem_limit_bytes=VMEM_LIMIT)


def forward_tiles(x, w_gate, w_up, w_down, plan):
    rows, width = x.shape
    mid = w_gate.shape[2]
    wide = pl.BlockSpec((TILE, width), lambda t, exp, at, own, *_: (at[t], 0))
    thin = pl.BlockSpec((TILE, mid), lambda t, exp, at, own, *_: (at[t], 0))
    owned = pl.BlockSpec((TILE, width), lambda t, exp, at, own, *_: (own[t], 0))
    w_in = pl.BlockSpec((1, width, mid), lambda t, exp, *_: (exp[t], 0, 0))
    w_out = pl.BlockSpec((1, mid, width), lambda t, exp, *_: (exp[t], 0, 0))
    return pl.pallas_call(
        forward_kernel,
        out_shape=[
            jax.ShapeDtypeStruct((rows, mid), jnp.float32),
            jax.ShapeDtypeStruct((rows, mid), jnp.float32),
            jax.ShapeDtypeStruct((rows, mid), jnp.bfloat16),
            jax.ShapeDtypeStruct((rows, width), jnp.bfloat16),
        ],
        grid_spec=pltpu.PrefetchScalarGridSpec(num_scalar_prefetch=5, grid=(rows // TILE,), in_specs=[wide, w_in, w_in, w_out], out_specs=[thin, thin, thin, owned]),
        compiler_params=kernel_params(),
        cost_estimate=pl.CostEstimate(flops=120_000_000_000, bytes_accessed=250_000_000, transcendentals=0),
        name="forward_tiles",
    )(plan["tile_weight"], plan["tile_at"], plan["own_at"], plan["tile_kind"], plan["own_kind"], x, w_gate, w_up, w_down)


def inward_tiles(d_rows, act_gate, act_up, w_gate, w_up, w_down, plan, begun):
    own = begun is None
    rows, width = d_rows.shape
    mid = w_gate.shape[2]
    wide = pl.BlockSpec((TILE, width), lambda t, exp, at, *_: (at[t], 0))
    thin = pl.BlockSpec((TILE, mid), lambda t, exp, at, *_: (at[t], 0))
    w_in = pl.BlockSpec((1, width, mid), lambda t, exp, *_: (exp[t], 0, 0))
    w_out = pl.BlockSpec((1, mid, width), lambda t, exp, *_: (exp[t], 0, 0))
    kept = pl.BlockSpec(memory_space=pl.ANY)
    thin_shape = jax.ShapeDtypeStruct((rows, mid), jnp.bfloat16)
    seq = plan["own_seq"] if own else plan["other_seq"]
    return pl.pallas_call(
        functools.partial(inward_kernel, own),
        out_shape=[thin_shape, thin_shape] + ([jax.ShapeDtypeStruct((rows, width), jnp.bfloat16)] if own else []),
        grid_spec=pltpu.PrefetchScalarGridSpec(
            num_scalar_prefetch=3,
            grid=(seq[0].shape[0],),
            in_specs=[wide, thin, thin] + ([w_in, w_in, w_out] if own else [w_out, kept, kept]),
            out_specs=[thin, thin] + ([wide] if own else []),
        ),
        input_output_aliases={} if own else {7: 0, 8: 1},
        compiler_params=kernel_params(),
        cost_estimate=pl.CostEstimate(flops=90_000_000_000 if own else 45_000_000_000, bytes_accessed=150_000_000, transcendentals=0),
        name="inward_own" if own else "inward_other",
    )(*seq, d_rows, act_gate, act_up, *((w_gate, w_up, w_down) if own else (w_down, *begun)))


def grad_tiles(lefts, left_arrays, right_arrays, plan):
    n_exp = plan["tail_at"].shape[0]
    rows = plan["tile_at"].shape[0] * TILE
    shapes = [(left_arrays[which].shape[1], right.shape[1]) for which, right in zip(lefts, right_arrays)]
    in_specs = [pl.BlockSpec((TILE, array.shape[1]), lambda t, exp, at, *_: (at[t], 0)) for array in (*left_arrays, *right_arrays)]
    alone = [pl.BlockSpec((1, *shape), lambda t, exp, *_: (exp[t], 0, 0)) for shape in shapes]
    whole = [pl.BlockSpec((1, *shape), lambda t, exp, at, kind, first, last, base: (base[0] + exp[t], 0, 0)) for shape in shapes]
    return pl.pallas_call(
        functools.partial(grads_kernel, lefts),
        out_shape=[jax.ShapeDtypeStruct((n_exp, *shape), jnp.bfloat16) for shape in shapes]
        + [jax.ShapeDtypeStruct((2 * n_exp, *shape), jnp.bfloat16) for shape in shapes],
        grid_spec=pltpu.PrefetchScalarGridSpec(
            num_scalar_prefetch=6,
            grid=(rows // TILE,),
            in_specs=in_specs,
            out_specs=alone + whole,
            scratch_shapes=[pltpu.VMEM(shape, jnp.float32) for shape in shapes],
        ),
        compiler_params=kernel_params(),
        cost_estimate=pl.CostEstimate(flops=45_000_000_000 * len(lefts), bytes_accessed=100_000_000 * len(lefts), transcendentals=0),
    )(plan["tile_exp"], plan["tile_at"], plan["tile_kind"], plan["tile_first"], plan["tile_last"], plan["base"], *left_arrays, *right_arrays)


def merge_kernel(base, whole_in, other, whole):
    whole[...] = other[...]


def merge(whole, other, other_base):
    n_exp, *shape = other.shape
    return pl.pallas_call(
        merge_kernel,
        out_shape=jax.ShapeDtypeStruct(whole.shape, whole.dtype),
        grid_spec=pltpu.PrefetchScalarGridSpec(
            num_scalar_prefetch=1,
            grid=(n_exp,),
            in_specs=[pl.BlockSpec(memory_space=pl.ANY), pl.BlockSpec((1, *shape), lambda i, base: (i, 0, 0))],
            out_specs=pl.BlockSpec((1, *shape), lambda i, base: (base[0] + i, 0, 0)),
        ),
        input_output_aliases={1: 0},
        compiler_params=pltpu.CompilerParams(dimension_semantics=("arbitrary",), vmem_limit_bytes=16 * 1024 * 1024),
        cost_estimate=pl.CostEstimate(flops=8_000_000_000, bytes_accessed=30_000_000, transcendentals=0),
        name="merge",
    )(other_base, whole, other)


def exclusive(values, axis=0):
    return jnp.cumsum(values, axis=axis) - values


def make_plan(local_ids, order, own_blocks, n_exp, max_tiles, weight_base):
    onehot = (local_ids[:, :, None, :] == jnp.arange(n_exp)[None, None, :, None]).astype(jnp.float32)
    hits = jnp.sum(onehot, axis=1)
    before = jnp.triu(jnp.ones((BLOCK, BLOCK), jnp.bfloat16), 1)
    rank = jnp.einsum("oet,ts->oes", hits.astype(jnp.bfloat16), before, preferred_element_type=jnp.float32)
    seg_len = (jnp.sum(hits, axis=2).astype(jnp.int32) + GROUP - 1) // GROUP
    seg_src = exclusive(seg_len, 1)
    per_tile, per_half = TILE // GROUP, HALF // GROUP
    groups = jnp.sum(seg_len, axis=0)
    tiles = (groups + per_tile - 1) // per_tile
    tile_base = exclusive(tiles)
    seg_dst = tile_base[None, :] * per_tile + exclusive(seg_len, 0)
    place = rank + (seg_src * GROUP).astype(jnp.float32)[:, :, None]
    pos = jnp.sum(onehot * (place[:, None] + 1.0), axis=2).astype(jnp.int32) - 1
    own_tiles = (jnp.sum(seg_len[:own_blocks], axis=0) + per_tile - 1) // per_tile
    exp_ids = jnp.arange(n_exp)

    def sequence(counts, length):
        ids = jnp.arange(length)
        at = jnp.minimum(ids, jnp.maximum(jnp.sum(counts) - 1, 0))
        ends = jnp.cumsum(counts)
        exp = jnp.minimum(jnp.sum((at[:, None] >= ends[None, :]).astype(jnp.int32), axis=1), n_exp - 1)
        is_exp = (exp[:, None] == exp_ids[None, :]).astype(jnp.int32)
        pick = lambda table: jnp.sum(is_exp * table[None, :], axis=1)
        return exp, at - pick(ends - counts), ids > at, pick

    def kind_of(pick, nth, past):
        left = pick(groups) - nth * per_tile
        return jnp.where(past, 0, jnp.where(left <= per_half, 1, 2))

    exp, nth, past, pick = sequence(tiles, max_tiles)
    kind = kind_of(pick, nth, past)
    own_count = pick(own_tiles)
    max_own = n_exp * (max_tiles // n_exp // 2 + 1)
    o_exp, o_nth, o_past, o_pick = sequence(own_tiles, max_own)
    r_exp, r_nth, r_past, r_pick = sequence(tiles - own_tiles, max_tiles)
    none = jnp.sum(tiles - own_tiles) == 0
    r_exp = jnp.where(none, 0, r_exp)
    r_nth = jnp.where(none, 0, r_nth + r_pick(own_tiles))
    r_kind = jnp.where(none, jnp.where(r_past, 0, jnp.where(groups[0] <= per_half, 1, 2)), kind_of(r_pick, r_nth, r_past))
    r_tile = jnp.where(none, 0, r_pick(tile_base) + r_nth)
    stack_rows = jnp.sum(seg_len, axis=1) * GROUP
    plan = {
        "order": order,
        "n_chunk": (stack_rows + CHUNK - 1) // CHUNK,
        "n_mix": (stack_rows + MIX - 1) // MIX,
        "seg_len": seg_len.reshape(-1),
        "seg_src": seg_src.reshape(-1),
        "seg_dst": seg_dst.reshape(-1),
        "tail_at": tile_base * per_tile + groups,
        "tail_len": (groups + per_half - 1) // per_half * per_half - groups,
        "base": weight_base.reshape(1),
        "tile_exp": exp,
        "tile_weight": exp + weight_base,
        "tile_at": pick(tile_base) + nth,
        "own_at": pick(tile_base) + jnp.minimum(nth, own_count - 1),
        "tile_kind": kind,
        "own_kind": jnp.where(nth < own_count, kind, 0),
        "tile_first": (nth == 0) & ~past,
        "tile_last": (nth == pick(tiles) - 1) & ~past,
        "own_seq": (o_exp + weight_base, o_pick(tile_base) + o_nth, kind_of(o_pick, o_nth, o_past)),
        "other_seq": (r_exp + weight_base, r_tile, r_kind),
    }
    return jax.tree.map(lambda value: value.astype(jnp.int32), plan), pos


def solution(mesh):
    ep_size = mesh.shape["ep"]
    dp_size = mesh.shape["dp"]
    devices = ep_size * dp_size
    cores = 2
    tok_spec = P(("dp", "ep"), None)
    exp_spec = P("ep", None, None)
    core_perm = [(i, i ^ 1) for i in range(dp_size)]
    ep_perm = [(i, i ^ 1) for i in range(ep_size)]

    def to_core(away):
        return lax.ppermute(away, "dp", core_perm)

    def to_ep(far):
        return lax.ppermute(far, "ep", ep_perm)

    def after(value, other):
        return lax.optimization_barrier((value, other))

    def device_step(tokens, d_out, expert_ids, norm_gain, router, w_gate, w_up, w_down):
        tok_rows, _ = tokens.shape
        top_k = expert_ids.shape[1]
        local_experts = w_gate.shape[0]
        experts = local_experts * ep_size
        total_tok = tok_rows * devices
        n_exp = local_experts // cores
        dev_blocks = tok_rows // BLOCK
        own_devs = devices // 2
        own_blocks = own_devs * dev_blocks
        seg_pad = devices * dev_blocks * (GROUP - 1)
        max_tiles = n_exp * -(-(devices * MAX_HITS + seg_pad) // TILE)

        ep_at = lax.axis_index("ep")
        dp_at = lax.axis_index("dp")
        core_at = lax.rem(dp_at, cores)
        x_at = lax.div(dp_at, cores)

        def dev_of(x, core, ep):
            return (x * cores + core) * ep_size + ep

        dev_order = jnp.stack(
            [dev_of(x_at, 1 - core_at, 1 - ep_at), dev_of(x_at, 1 - core_at, ep_at), dev_of(x_at, core_at, 1 - ep_at), dev_of(x_at, core_at, ep_at)]
            + [dev_of(1 - x_at, core, ep) for core in range(cores) for ep in range(ep_size)]
        )
        order = (dev_order[:, None] * dev_blocks + jnp.arange(dev_blocks)[None, :]).reshape(-1).astype(jnp.int32)

        tokens32 = tokens.astype(jnp.float32)
        gain32 = norm_gain.astype(jnp.float32)
        inv_rms, normed = norm_forward(tokens32, gain32)
        logits = jnp.dot(normed, router, preferred_element_type=jnp.float32)
        router_probs = jax.nn.softmax(logits, axis=1)
        expert_hits = expert_ids[:, :, None] == jnp.arange(experts)[None, None, :]
        gate_vals = jnp.sum(jnp.where(expert_hits, router_probs[:, None, :], 0.0), axis=2)

        prob_sums = jnp.pad(jnp.sum(router_probs, axis=0), (0, tok_rows - experts))
        packet = jnp.concatenate([expert_ids.astype(jnp.float32).T, gate_vals.T, prob_sums[None]], axis=0)
        packets = lax.all_gather(packet, ("dp", "ep"))
        all_normed = lax.all_gather(normed, ("dp", "ep"), tiled=True)
        d_out_late, _ = lax.optimization_barrier((d_out, all_normed[:8]))
        all_d_out = lax.all_gather(d_out_late, ("dp", "ep"), tiled=True)

        all_ids = packets[:, :top_k].astype(jnp.int32)
        counts = jnp.sum((all_ids[..., None] == jnp.arange(experts)).astype(jnp.float32), axis=(0, 1, 2))
        expert_frac = counts / (total_tok * top_k)
        aux_loss = AUX_COEF * experts * jnp.sum(expert_frac * jnp.sum(packets[:, 2 * top_k, :experts], axis=0)) / total_tok

        turned = jnp.take(packets, dev_order, axis=0)

        def by_block(rows):
            return rows.reshape(devices, top_k, dev_blocks, BLOCK).transpose(0, 2, 1, 3).reshape(devices * dev_blocks, top_k, BLOCK)

        first_expert = ep_at * local_experts + core_at * n_exp
        block_ids = by_block(turned[:, :top_k]).astype(jnp.int32) - first_expert
        block_ids = jnp.where((block_ids >= 0) & (block_ids < n_exp), block_ids, n_exp)
        block_gates = by_block(turned[:, top_k:2 * top_k])
        plan, pos = make_plan(block_ids, order, own_blocks, n_exp, max_tiles, core_at * n_exp)
        pos_t = pos[:own_blocks].transpose(0, 2, 1)
        gates_t = block_gates[:own_blocks].transpose(0, 2, 1)

        rows = max_tiles * TILE
        x = dispatch(all_normed, pos, block_gates, plan, rows, False)
        act_gate, act_up, hidden, result = forward_tiles(x, w_gate, w_up, w_down, plan)
        away, far, near, d_gate_parts = combine(result, pos_t, gates_t, all_d_out, plan, True)
        all_d_out, away = after(all_d_out, away)
        met = to_core(away)
        half, quarter = own_blocks // 2, own_blocks // 4
        d_gate_met = to_core(d_gate_parts[:half])
        d_rows = dispatch(all_d_out, pos, block_gates, plan, rows, True)
        d_gate_mine = d_gate_parts[half:] + d_gate_met
        d_rows, (far, d_gate_far) = after(d_rows, (far + met[:tok_rows], d_gate_mine[:quarter]))
        crossed = to_ep(far)
        d_gate_crossed = to_ep(d_gate_far)
        d_act_gate, d_act_up, d_expert_in = inward_tiles(d_rows, act_gate, act_up, w_gate, w_up, w_down, plan, None)
        d_away, d_far, d_near = combine(d_expert_in, pos_t, gates_t, all_d_out, plan, False)
        d_act_gate, d_away = after(d_act_gate, d_away)
        d_met = to_core(d_away)
        d_gates = (d_gate_mine[quarter:] + d_gate_crossed).reshape(tok_rows, top_k)
        d_probs = jnp.sum(jnp.where(expert_hits, d_gates[:, :, None], 0.0), axis=1) + (AUX_COEF * experts / total_tok) * expert_frac[None, :]
        d_logits = (router_probs * (d_probs - jnp.sum(router_probs * d_probs, axis=1, keepdims=True))).astype(jnp.bfloat16)
        grad_router = lax.dot_general(normed, d_logits, TN_DIMS, preferred_element_type=jnp.float32)
        d_act_gate, d_act_up = inward_tiles(d_rows, act_gate, act_up, w_gate, w_up, w_down, plan, (d_act_gate, d_act_up))
        d_act_gate, (d_far, grad_router) = after(d_act_gate, (d_far + d_met[:tok_rows], grad_router))
        d_crossed = to_ep(d_far)
        grad_router = lax.psum(grad_router, ("ep", "dp"))
        grad_gate, grad_up, all_gate, all_up = grad_tiles((0, 0), (x,), (d_act_gate, d_act_up), plan)
        hidden, grad_gate = after(hidden, grad_gate)
        grad_down, all_down = grad_tiles((0,), (hidden,), (d_rows,), plan)
        other_base = (1 - core_at).reshape(1).astype(jnp.int32) * n_exp
        all_gate = merge(all_gate, to_core(grad_gate), other_base)
        all_up = merge(all_up, to_core(grad_up), other_base)
        all_down = merge(all_down, to_core(grad_down), other_base)
        layer_out = (tokens32 + (near + met[tok_rows:] + crossed)).astype(jnp.bfloat16)
        d_normed = (d_near + d_met[tok_rows:] + d_crossed) + lax.dot_general(d_logits, router, NT_DIMS, preferred_element_type=jnp.float32)
        d_tokens = (d_out.astype(jnp.float32) + norm_backward(tokens32, inv_rms, gain32, d_normed)).astype(jnp.bfloat16)
        return layer_out, aux_loss.reshape(1), d_tokens, grad_router, all_gate, all_up, all_down

    return jax.shard_map(device_step, mesh=mesh, in_specs=(tok_spec, tok_spec, tok_spec, P(None), P(None, None), exp_spec, exp_spec, exp_spec), out_specs=(tok_spec, P(None), tok_spec, P(None, None), exp_spec, exp_spec, exp_spec), check_vma=False)
```

```python
import functools

import jax
import jax.numpy as jnp
from jax import lax
from jax.experimental import pallas as pl
from jax.experimental.pallas import tpu as pltpu
from jax.sharding import PartitionSpec as P


AUX_COEF = 0.001
NORM_EPS = 1e-6
MAX_HITS = 416
BLOCK = 256
GROUP = 16
TILE = 512
HALF = TILE // 2
CHUNK = 256
MIX = 256
NT_DIMS = (((1,), (1,)), ((), ()))
TN_DIMS = (((0,), (0,)), ((), ()))
VMEM_LIMIT = 60 * 1024 * 1024


def norm_forward(tokens32, gain32):
    inv_rms = lax.rsqrt(jnp.mean(tokens32 * tokens32, axis=1, keepdims=True) + NORM_EPS)
    return inv_rms, (tokens32 * inv_rms * gain32).astype(jnp.bfloat16)


def norm_backward(tokens32, inv_rms, gain32, d_normed):
    d_scaled = d_normed * gain32
    return inv_rms * (d_scaled - tokens32 * (inv_rms * inv_rms) * jnp.mean(d_scaled * tokens32, axis=1, keepdims=True))


def dot32(left, right, dims=(((1,), (0,)), ((), ()))):
    return lax.dot_general(left, right, dims, preferred_element_type=jnp.float32)


def dispatch_kernel(scaled, begun, n_exp, src_blk, ordinal, n_chunk, seg_len, seg_src, seg_dst, tail_at, tail_len, src, pos, gates, *rest):
    out, stack, blank, sems, tail_sem = rest[1:] if begun else rest
    step = pl.program_id(0)
    last = pl.num_programs(0) - 1
    slot = lax.rem(step, 2)

    def segment_copy(blk, buf, exp, grp):
        at = blk * n_exp + exp
        from_row = pl.multiple_of((seg_src[at] + grp) * GROUP, GROUP)
        to_row = pl.multiple_of((seg_dst[at] + grp) * GROUP, GROUP)
        return pltpu.make_async_copy(stack.at[buf, pl.ds(from_row, GROUP), :], out.at[pl.ds(to_row, GROUP), :], sems.at[buf])

    def each_segment(blk, buf, act):
        for exp in range(n_exp):
            @pl.loop(0, seg_len[blk * n_exp + exp])
            def _(grp):
                act(segment_copy(blk, buf, exp, grp))

    def each_tail(act):
        for exp in range(n_exp):
            @pl.loop(0, tail_len[exp])
            def _(grp):
                to_row = pl.multiple_of((tail_at[exp] + grp) * GROUP, GROUP)
                act(pltpu.make_async_copy(blank, out.at[pl.ds(to_row, GROUP), :], tail_sem))

    if not begun:
        @pl.when(step == 0)
        def _():
            blank[...] = jnp.zeros_like(blank)
            each_tail(lambda copy: copy.start())

    @pl.when(step >= 2)
    def _():
        each_segment(ordinal[step - 2], slot, lambda copy: copy.wait())

    @pl.loop(0, n_chunk[ordinal[step]])
    def _(chunk):
        row = lax.broadcasted_iota(jnp.int32, (CHUNK, BLOCK), 0) + chunk * CHUNK
        hit = pos[0, 0:1, :] == row
        if scaled:
            weight = jnp.where(hit, gates[0, 0:1, :], 0.0)
        for k in range(1, pos.shape[1]):
            here = pos[0, k:k + 1, :] == row
            hit = jnp.logical_or(hit, here)
            if scaled:
                weight = jnp.where(here, gates[0, k:k + 1, :], weight)
        picked = dot32(jnp.where(hit, 1.0, 0.0).astype(jnp.bfloat16), src[...])
        if scaled:
            picked = picked * jnp.sum(weight, axis=1, keepdims=True)
        stack[slot, pl.ds(pl.multiple_of(chunk * CHUNK, CHUNK), CHUNK), :] = picked.astype(jnp.bfloat16)

    each_segment(ordinal[step], slot, lambda copy: copy.start())

    @pl.when(step == last)
    def _():
        each_segment(ordinal[step - 1], 1 - slot, lambda copy: copy.wait())
        each_segment(ordinal[step], slot, lambda copy: copy.wait())
        if not begun:
            each_tail(lambda copy: copy.wait())


def dispatch(src, pos, gates, plan, part, out, rows, scaled):
    top_k = pos.shape[1]
    src_blk, ordinal = plan["parts"][part]
    begun = out is not None
    width = src.shape[1]
    n_exp = plan["tail_at"].shape[0]
    stack_rows = -(-(BLOCK * top_k + n_exp * (GROUP - 1)) // CHUNK) * CHUNK
    return pl.pallas_call(
        functools.partial(dispatch_kernel, scaled, begun, n_exp),
        out_shape=jax.ShapeDtypeStruct((rows, width), jnp.bfloat16),
        grid_spec=pltpu.PrefetchScalarGridSpec(
            num_scalar_prefetch=8,
            grid=(ordinal.shape[0],),
            in_specs=[
                pl.BlockSpec((BLOCK, width), lambda i, blk, *_: (blk[i], 0)),
                pl.BlockSpec((1, top_k, BLOCK), lambda i, blk, ordinal, *_: (ordinal[i], 0, 0)),
                pl.BlockSpec((1, top_k, BLOCK), lambda i, blk, ordinal, *_: (ordinal[i], 0, 0)),
            ]
            + [pl.BlockSpec(memory_space=pl.ANY)] * begun,
            out_specs=pl.BlockSpec(memory_space=pl.ANY),
            scratch_shapes=[
                pltpu.VMEM((2, stack_rows, width), jnp.bfloat16),
                pltpu.VMEM((GROUP, width), jnp.bfloat16),
                pltpu.SemaphoreType.DMA((2,)),
                pltpu.SemaphoreType.DMA,
            ],
        ),
        compiler_params=pltpu.CompilerParams(dimension_semantics=("arbitrary",), vmem_limit_bytes=VMEM_LIMIT),
        input_output_aliases={11: 0} if begun else {},
        cost_estimate=pl.CostEstimate(flops=20_000_000_000, bytes_accessed=80_000_000, transcendentals=0),
        name="dispatch_scaled" if scaled else "dispatch",
    )(src_blk, ordinal, plan["n_chunk"], plan["seg_len"], plan["seg_src"], plan["seg_dst"], plan["tail_at"], plan["tail_len"], src, pos, gates, *([out] * begun))


def combine_kernel(weighted, first, counts, dev_blocks, n_exp, at0, at1, n_mix, seg_len, seg_src, seg_dst, rows, pos, gates, *rest):
    if weighted:
        d_out0, d_out1, *outs, d_gates, stack, total, sems = rest
    else:
        *outs, stack, total, sems = rest
    step = pl.program_id(0)
    blocks = pl.num_programs(0)
    slot = lax.rem(step, 2)

    def each_segment(blk, buf, act):
        for exp in range(n_exp):
            @pl.loop(0, seg_len[blk * n_exp + exp])
            def _(grp):
                at = blk * n_exp + exp
                to_row = pl.multiple_of((seg_src[at] + grp) * GROUP, GROUP)
                from_row = pl.multiple_of((seg_dst[at] + grp) * GROUP, GROUP)
                act(pltpu.make_async_copy(rows.at[pl.ds(from_row, GROUP), :], stack.at[buf, pl.ds(to_row, GROUP), :], sems.at[buf]))

    @pl.when(step == 0)
    def _():
        @pl.loop(0, stack.shape[1] // MIX)
        def _(part):
            stack[:, pl.ds(pl.multiple_of(part * MIX, MIX), MIX), :] = jnp.zeros((2, MIX, stack.shape[2]), stack.dtype)

        each_segment(first, 0, lambda copy: copy.start())

    @pl.when(step < blocks - 1)
    def _():
        each_segment(first + step + 1, 1 - slot, lambda copy: copy.start())

    each_segment(first + step, slot, lambda copy: copy.wait())
    total[...] = jnp.zeros_like(total)
    if weighted:
        d_gates[...] = jnp.zeros_like(d_gates)

    @pl.loop(0, n_mix[first + step])
    def _(part):
        col = lax.broadcasted_iota(jnp.int32, (BLOCK, MIX), 1) + part * MIX
        part_rows = stack[slot, pl.ds(pl.multiple_of(part * MIX, MIX), MIX), :]
        top_k = pos.shape[2]
        if weighted:
            late = lax.rem(step, dev_blocks) >= dev_blocks // 2
            cross = dot32(jnp.where(late, d_out1[...], d_out0[...]), part_rows, NT_DIMS)
            weight = jnp.zeros((BLOCK, MIX), jnp.float32)
            d_cols = []
            for k in range(top_k):
                here = pos[0, :, k:k + 1] == col
                weight = jnp.where(here, gates[0, :, k:k + 1], weight)
                d_cols.append(jnp.sum(jnp.where(here, cross, 0.0), axis=1, keepdims=True))
            d_gates[0] += jnp.concatenate(d_cols, axis=1)
            high = weight.astype(jnp.bfloat16)
            left = weight - high.astype(jnp.float32)
            mid = left.astype(jnp.bfloat16)
            low = (left - mid.astype(jnp.float32)).astype(jnp.bfloat16)
            mixed = dot32(jnp.concatenate([high, mid, low], axis=0), part_rows)
            total[...] += mixed[:BLOCK] + mixed[BLOCK:2 * BLOCK] + mixed[2 * BLOCK:]
        else:
            hit = pos[0, :, 0:1] == col
            for k in range(1, top_k):
                hit = jnp.logical_or(hit, pos[0, :, k:k + 1] == col)
            total[...] += dot32(jnp.where(hit, 1.0, 0.0).astype(jnp.bfloat16), part_rows)

    begin = 0
    for out, count in zip(outs, counts):
        @pl.when((step >= begin) & (step < begin + count))
        def _():
            out[...] = total[...]

        begin += count


def combine(rows, pos_t, gates_t, d_outs, plan, first, counts, weighted):
    _, _, top_k = pos_t.shape
    width = rows.shape[1]
    n_exp = plan["tail_at"].shape[0]
    blocks = sum(counts)
    stack_rows = -(-(BLOCK * top_k + n_exp * (GROUP - 1)) // MIX) * MIX
    out_shape, out_specs, begin = [], [], 0
    for count in counts:
        out_shape.append(jax.ShapeDtypeStruct((count * BLOCK, width), jnp.float32))
        out_specs.append(pl.BlockSpec((BLOCK, width), lambda i, *_, begin=begin, count=count: (jnp.clip(i - begin, 0, count - 1), 0)))
        begin += count
    d_specs = []
    if weighted:
        out_shape.append(jax.ShapeDtypeStruct((blocks, BLOCK, top_k), jnp.float32))
        out_specs.append(pl.BlockSpec((1, BLOCK, top_k), lambda i, *_: (i, 0, 0)))
        d_specs = [
            pl.BlockSpec((BLOCK, width), lambda i, at0, at1, *_: (at0[first + i], 0)),
            pl.BlockSpec((BLOCK, width), lambda i, at0, at1, *_: (at1[first + i], 0)),
        ]
    return pl.pallas_call(
        functools.partial(combine_kernel, weighted, first, counts, plan["dev_blocks"], n_exp),
        out_shape=out_shape,
        grid_spec=pltpu.PrefetchScalarGridSpec(
            num_scalar_prefetch=6,
            grid=(blocks,),
            in_specs=[
                pl.BlockSpec(memory_space=pl.ANY),
                pl.BlockSpec((1, BLOCK, top_k), lambda i, *_: (first + i, 0, 0)),
                pl.BlockSpec((1, BLOCK, top_k), lambda i, *_: (first + i, 0, 0)),
            ]
            + d_specs,
            out_specs=out_specs,
            scratch_shapes=[
                pltpu.VMEM((2, stack_rows, width), jnp.bfloat16),
                pltpu.VMEM((BLOCK, width), jnp.float32),
                pltpu.SemaphoreType.DMA((2,)),
            ],
        ),
        compiler_params=pltpu.CompilerParams(dimension_semantics=("arbitrary",), vmem_limit_bytes=VMEM_LIMIT),
        cost_estimate=pl.CostEstimate(flops=5_000_000_000 * blocks, bytes_accessed=60_000_000, transcendentals=0),
        name="combine_weighted" if weighted else "combine",
    )(*plan["d_at"], plan["n_mix"], plan["seg_len"], plan["seg_src"], plan["seg_own"], rows, pos_t, gates_t, *(d_outs if weighted else ()))


def by_kind(kind, body):
    for code, rows in ((1, HALF), (2, TILE)):
        @pl.when(kind == code)
        def _():
            body(pl.ds(0, rows))


def activations(x, w_gate, w_up):
    a = dot32(x, w_gate)
    b = dot32(x, w_up)
    sig = jax.nn.sigmoid(a)
    return a, b, sig, (a * sig * b).astype(jnp.bfloat16)


def cotangents(d_rows, w_down, a, b, sig):
    d_hidden = dot32(d_rows, w_down, NT_DIMS)
    d_a = (d_hidden * b * sig * (1.0 + a * (1.0 - sig))).astype(jnp.bfloat16)
    return d_a, (d_hidden * (a * sig)).astype(jnp.bfloat16)


def own_kernel(tile_exp, tile_at, own_at, tile_kind, x, d_rows, w_gate, w_up, w_down, hidden, d_gate, d_up, result, d_in):
    @pl.loop(0, tile_kind[pl.program_id(0)])
    def _(half):
        part = pl.ds(pl.multiple_of(half * HALF, HALF), HALF)
        a, b, sig, u = activations(x[part], w_gate[0], w_up[0])
        hidden[part] = u
        result[part] = dot32(u, w_down[0]).astype(jnp.bfloat16)
        d_a, d_b = cotangents(d_rows[part], w_down[0], a, b, sig)
        d_gate[part] = d_a
        d_up[part] = d_b
        d_in[part] = (dot32(d_a, w_gate[0], NT_DIMS) + dot32(d_b, w_up[0], NT_DIMS)).astype(jnp.bfloat16)


def rest_kernel(begun, tile_exp, tile_at, own_at, own_kind, other_kind, tile_first, tile_last, base, x, d_rows, w_gate, w_up, w_down, hidden, d_gate, d_up, *refs):
    g_gate, g_up, g_down, all_gate, all_up, all_down, s_gate, s_up, s_down, t_hidden, t_gate, t_up = refs[3:] if begun else refs
    step = pl.program_id(0)

    @pl.when(tile_first[step] > 0)
    def _():
        for total in (s_gate, s_up, s_down):
            total[...] = jnp.zeros_like(total)

    def add(u, d_a, d_b, part):
        s_gate[...] += dot32(x[part], d_a[part], TN_DIMS)
        s_up[...] += dot32(x[part], d_b[part], TN_DIMS)
        s_down[...] += dot32(u[part], d_rows[part], TN_DIMS)

    @pl.loop(0, other_kind[step])
    def _(half):
        part = pl.ds(pl.multiple_of(half * HALF, HALF), HALF)
        a, b, sig, u = activations(x[part], w_gate[0], w_up[0])
        t_hidden[part] = u
        t_gate[part], t_up[part] = cotangents(d_rows[part], w_down[0], a, b, sig)

    by_kind(own_kind[step], functools.partial(add, hidden, d_gate, d_up))
    by_kind(other_kind[step], functools.partial(add, t_hidden, t_gate, t_up))

    @pl.when(tile_last[step] > 0)
    def _():
        for out, whole, total in ((g_gate, all_gate, s_gate), (g_up, all_up, s_up), (g_down, all_down, s_down)):
            rounded = total[...].astype(jnp.bfloat16)
            out[0] = rounded
            whole[0] = rounded


def kernel_params():
    return pltpu.CompilerParams(dimension_semantics=("arbitrary",), vmem_limit_bytes=VMEM_LIMIT)


def own_tiles(x, d_rows, w_gate, w_up, w_down, plan):
    width = x.shape[1]
    mid = w_gate.shape[2]
    wide = pl.BlockSpec((TILE, width), lambda t, exp, at, *_: (at[t], 0))
    thin = pl.BlockSpec((TILE, mid), lambda t, exp, at, own, *_: (own[t], 0))
    wide_own = pl.BlockSpec((TILE, width), lambda t, exp, at, own, *_: (own[t], 0))
    w_in = pl.BlockSpec((1, width, mid), lambda t, exp, *_: (exp[t], 0, 0))
    w_out = pl.BlockSpec((1, mid, width), lambda t, exp, *_: (exp[t], 0, 0))
    seq = plan["own_seq"]
    own_rows = seq[0].shape[0] * TILE
    thin_shape = jax.ShapeDtypeStruct((own_rows, mid), jnp.bfloat16)
    wide_shape = jax.ShapeDtypeStruct((own_rows, width), jnp.bfloat16)
    return pl.pallas_call(
        own_kernel,
        out_shape=[thin_shape] * 3 + [wide_shape] * 2,
        grid_spec=pltpu.PrefetchScalarGridSpec(num_scalar_prefetch=4, grid=(seq[0].shape[0],), in_specs=[wide, wide, w_in, w_in, w_out], out_specs=[thin] * 3 + [wide_own] * 2),
        compiler_params=kernel_params(),
        cost_estimate=pl.CostEstimate(flops=120_000_000_000, bytes_accessed=250_000_000, transcendentals=0),
        name="own_tiles",
    )(*seq, x, d_rows, w_gate, w_up, w_down)


def rest_tiles(x, d_rows, w_gate, w_up, w_down, hidden, d_gate, d_up, plan, half, begun):
    width, mid = w_gate.shape[1:]
    n_half = plan["tail_at"].shape[0] // 2
    seq = plan["rest_seq"][half]
    shapes = [(width, mid), (width, mid), (mid, width)]
    wide = pl.BlockSpec((TILE, width), lambda t, exp, at, *_: (at[t], 0))
    kept = pl.BlockSpec((TILE, mid), lambda t, exp, at, own, *_: (own[t], 0))
    w_in = pl.BlockSpec((1, width, mid), lambda t, exp, at, own, k1, k2, first, last, base: (base[0] + exp[t], 0, 0))
    w_out = pl.BlockSpec((1, mid, width), lambda t, exp, at, own, k1, k2, first, last, base: (base[0] + exp[t], 0, 0))
    alone = [pl.BlockSpec((1, *shape), lambda t, exp, *_: (exp[t] - half * n_half, 0, 0)) for shape in shapes]
    return pl.pallas_call(
        functools.partial(rest_kernel, begun is not None),
        out_shape=[jax.ShapeDtypeStruct((n_half, *shape), jnp.bfloat16) for shape in shapes]
        + [jax.ShapeDtypeStruct((4 * n_half, *shape), jnp.bfloat16) for shape in shapes],
        grid_spec=pltpu.PrefetchScalarGridSpec(
            num_scalar_prefetch=8,
            grid=(seq[0].shape[0],),
            in_specs=[wide, wide, w_in, w_in, w_out, kept, kept, kept] + [pl.BlockSpec(memory_space=pl.ANY)] * (3 if begun else 0),
            out_specs=alone + [w_in, w_in, w_out],
            scratch_shapes=[pltpu.VMEM(shape, jnp.float32) for shape in shapes] + [pltpu.VMEM((TILE, mid), jnp.bfloat16)] * 3,
        ),
        input_output_aliases={16: 3, 17: 4, 18: 5} if begun else {},
        compiler_params=kernel_params(),
        cost_estimate=pl.CostEstimate(flops=80_000_000_000, bytes_accessed=150_000_000, transcendentals=0),
        name="rest_tiles",
    )(*seq, plan["base"], x, d_rows, w_gate, w_up, w_down, hidden, d_gate, d_up, *(begun or ()))


def merge_kernel(base, whole_in, other, whole):
    whole[...] = other[...]


def merge(whole, other, other_base):
    count, *shape = other.shape
    return pl.pallas_call(
        merge_kernel,
        out_shape=jax.ShapeDtypeStruct(whole.shape, whole.dtype),
        grid_spec=pltpu.PrefetchScalarGridSpec(
            num_scalar_prefetch=1,
            grid=(count,),
            in_specs=[pl.BlockSpec(memory_space=pl.ANY), pl.BlockSpec((1, *shape), lambda i, base: (i, 0, 0))],
            out_specs=pl.BlockSpec((1, *shape), lambda i, base: (base[0] + i, 0, 0)),
        ),
        input_output_aliases={1: 0},
        compiler_params=pltpu.CompilerParams(dimension_semantics=("arbitrary",), vmem_limit_bytes=16 * 1024 * 1024),
        cost_estimate=pl.CostEstimate(flops=8_000_000_000, bytes_accessed=30_000_000, transcendentals=0),
        name="merge",
    )(other_base, whole, other)


def exclusive(values, axis=0):
    return jnp.cumsum(values, axis=axis) - values


def make_plan(local_ids, dev_order, own_blocks, n_exp, max_tiles, max_own, weight_base):
    order = jnp.arange(local_ids.shape[0])
    onehot = (local_ids[:, :, None, :] == jnp.arange(n_exp)[None, None, :, None]).astype(jnp.float32)
    hits = jnp.sum(onehot, axis=1)
    before = jnp.triu(jnp.ones((BLOCK, BLOCK), jnp.bfloat16), 1)
    rank = jnp.einsum("oet,ts->oes", hits.astype(jnp.bfloat16), before, preferred_element_type=jnp.float32)
    seg_len = (jnp.sum(hits, axis=2).astype(jnp.int32) + GROUP - 1) // GROUP
    seg_src = exclusive(seg_len, 1)
    per_tile, per_half = TILE // GROUP, HALF // GROUP
    groups = jnp.sum(seg_len, axis=0)
    tiles = (groups + per_tile - 1) // per_tile
    tile_base = exclusive(tiles)
    seg_dst = tile_base[None, :] * per_tile + exclusive(seg_len, 0)
    place = rank + (seg_src * GROUP).astype(jnp.float32)[:, :, None]
    pos = jnp.sum(onehot * (place[:, None] + 1.0), axis=2).astype(jnp.int32) - 1
    own_tiles = (jnp.sum(seg_len[:own_blocks], axis=0) + per_tile - 1) // per_tile
    exp_ids = jnp.arange(n_exp)

    def sequence(counts, length):
        ids = jnp.arange(length)
        at = jnp.minimum(ids, jnp.maximum(jnp.sum(counts) - 1, 0))
        ends = jnp.cumsum(counts)
        exp = jnp.minimum(jnp.sum((at[:, None] >= ends[None, :]).astype(jnp.int32), axis=1), n_exp - 1)
        is_exp = (exp[:, None] == exp_ids[None, :]).astype(jnp.int32)
        pick = lambda table: jnp.sum(is_exp * table[None, :], axis=1)
        return exp, at - pick(ends - counts), ids > at, pick

    def kind_of(pick, nth, past):
        left = pick(groups) - nth * per_tile
        return jnp.where(past, 0, jnp.where(left <= per_half, 1, 2))

    o_exp, o_nth, o_past, o_pick = sequence(own_tiles, max_own)
    own_base = exclusive(own_tiles)

    def rest_seq(half):
        mine = exp_ids // (n_exp // 2) == half
        exp, nth, past, pick = sequence(jnp.where(mine, tiles, 0), max_tiles // 2)
        kind = kind_of(pick, nth, past)
        own_count = pick(own_tiles)
        is_own = nth < own_count
        seq = (
            exp,
            pick(tile_base) + nth,
            pick(own_base) + jnp.minimum(nth, own_count - 1),
            jnp.where(is_own, kind, 0),
            jnp.where(is_own, 0, kind),
            (nth == 0) & ~past,
            (nth == pick(tiles) - 1) & ~past,
        )
        return seq

    dev_blocks = order.shape[0] // dev_order.shape[0]
    part_blocks = dev_blocks // 2
    in_part = jnp.arange(part_blocks)

    def part_of(part):
        blk = dev_order[:, None] * part_blocks + in_part[None, :]
        ordinal = jnp.arange(dev_order.shape[0])[:, None] * dev_blocks + part * part_blocks + in_part[None, :]
        return blk.reshape(-1), ordinal.reshape(-1)

    d_at = dev_order[:, None] * part_blocks + jnp.arange(dev_blocks)[None, :] % part_blocks
    early = jnp.arange(dev_blocks)[None, :] < part_blocks
    d_at0 = jnp.where(early, d_at, d_at[:, part_blocks - 1:part_blocks])
    d_at1 = jnp.where(early, d_at[:, :1], d_at)
    stack_rows = jnp.sum(seg_len, axis=1) * GROUP
    plan = {
        "parts": (part_of(0), part_of(1)),
        "d_at": (d_at0.reshape(-1), d_at1.reshape(-1)),
        "n_chunk": (stack_rows + CHUNK - 1) // CHUNK,
        "n_mix": (stack_rows + MIX - 1) // MIX,
        "seg_len": seg_len.reshape(-1),
        "seg_src": seg_src.reshape(-1),
        "seg_dst": seg_dst.reshape(-1),
        "seg_own": (own_base[None, :] * per_tile + exclusive(seg_len, 0)).reshape(-1),
        "tail_at": tile_base * per_tile + groups,
        "tail_len": (groups + per_half - 1) // per_half * per_half - groups,
        "base": weight_base.reshape(1),
        "own_seq": (o_exp + weight_base, o_pick(tile_base) + o_nth, o_pick(own_base) + o_nth, kind_of(o_pick, o_nth, o_past)),
        "rest_seq": (rest_seq(0), rest_seq(1)),
    }
    return jax.tree.map(lambda value: value.astype(jnp.int32), plan), pos


def solution(mesh):
    ep_size = mesh.shape["ep"]
    dp_size = mesh.shape["dp"]
    devices = ep_size * dp_size
    cores = 2
    tok_spec = P(("dp", "ep"), None)
    exp_spec = P("ep", None, None)
    core_perm = [(i, i ^ 1) for i in range(dp_size)]
    ep_perm = [(i, i ^ 1) for i in range(ep_size)]

    def to_core(away):
        return lax.ppermute(away, "dp", core_perm)

    def to_ep(far):
        return lax.ppermute(far, "ep", ep_perm)

    def after(value, other):
        return lax.optimization_barrier((value, other))

    def device_step(tokens, d_out, expert_ids, norm_gain, router, w_gate, w_up, w_down):
        tok_rows, _ = tokens.shape
        top_k = expert_ids.shape[1]
        local_experts = w_gate.shape[0]
        experts = local_experts * ep_size
        total_tok = tok_rows * devices
        n_exp = local_experts // cores
        dev_blocks = tok_rows // BLOCK
        own_devs = devices // 2
        own_blocks = own_devs * dev_blocks
        seg_pad = devices * dev_blocks * (GROUP - 1)
        max_own = n_exp * -(-(own_devs * MAX_HITS + own_blocks * (GROUP - 1)) // TILE)
        max_tiles = n_exp * -(-(devices * MAX_HITS + seg_pad) // TILE)

        ep_at = lax.axis_index("ep")
        dp_at = lax.axis_index("dp")
        core_at = lax.rem(dp_at, cores)
        x_at = lax.div(dp_at, cores)

        def dev_of(x, core, ep):
            return (x * cores + core) * ep_size + ep

        dev_order = jnp.stack(
            [dev_of(x_at, 1 - core_at, 1 - ep_at), dev_of(x_at, 1 - core_at, ep_at), dev_of(x_at, core_at, 1 - ep_at), dev_of(x_at, core_at, ep_at)]
            + [dev_of(1 - x_at, core, ep) for core in range(cores) for ep in range(ep_size)]
        )
        tokens32 = tokens.astype(jnp.float32)
        gain32 = norm_gain.astype(jnp.float32)
        inv_rms, normed = norm_forward(tokens32, gain32)
        logits = jnp.dot(normed, router, preferred_element_type=jnp.float32)
        router_probs = jax.nn.softmax(logits, axis=1)
        expert_hits = expert_ids[:, :, None] == jnp.arange(experts)[None, None, :]
        gate_vals = jnp.sum(jnp.where(expert_hits, router_probs[:, None, :], 0.0), axis=2)

        prob_sums = jnp.pad(jnp.sum(router_probs, axis=0), (0, tok_rows - experts))
        packet = jnp.concatenate([expert_ids.astype(jnp.float32).T, gate_vals.T, prob_sums[None]], axis=0)
        packets = lax.all_gather(packet, ("dp", "ep"))
        half_rows = tok_rows // 2
        parts = [normed[:half_rows], normed[half_rows:], d_out[:half_rows], d_out[half_rows:]]
        gathered = [lax.all_gather(parts[0], ("dp", "ep"), tiled=True)]
        for part in parts[1:]:
            late, _ = lax.optimization_barrier((part, gathered[-1][:8]))
            gathered.append(lax.all_gather(late, ("dp", "ep"), tiled=True))
        all_normed, all_d_out = gathered[:2], gathered[2:]

        all_ids = packets[:, :top_k].astype(jnp.int32)
        counts = jnp.sum((all_ids[..., None] == jnp.arange(experts)).astype(jnp.float32), axis=(0, 1, 2))
        expert_frac = counts / (total_tok * top_k)
        aux_loss = AUX_COEF * experts * jnp.sum(expert_frac * jnp.sum(packets[:, 2 * top_k, :experts], axis=0)) / total_tok

        turned = jnp.take(packets, dev_order, axis=0)

        def by_block(rows):
            return rows.reshape(devices, top_k, dev_blocks, BLOCK).transpose(0, 2, 1, 3).reshape(devices * dev_blocks, top_k, BLOCK)

        first_expert = ep_at * local_experts + core_at * n_exp
        block_ids = by_block(turned[:, :top_k]).astype(jnp.int32) - first_expert
        block_ids = jnp.where((block_ids >= 0) & (block_ids < n_exp), block_ids, n_exp)
        block_gates = by_block(turned[:, top_k:2 * top_k])
        plan, pos = make_plan(block_ids, dev_order, own_blocks, n_exp, max_tiles, max_own, core_at * n_exp)
        plan["dev_blocks"] = dev_blocks
        pos_t = pos[:own_blocks].transpose(0, 2, 1)
        gates_t = block_gates[:own_blocks].transpose(0, 2, 1)

        rows = max_tiles * TILE
        x = dispatch(all_normed[0], pos, block_gates, plan, 0, None, rows, False)
        x = dispatch(all_normed[1], pos, block_gates, plan, 1, x, rows, False)
        d_rows = dispatch(all_d_out[0], pos, block_gates, plan, 0, None, rows, True)
        d_rows = dispatch(all_d_out[1], pos, block_gates, plan, 1, d_rows, rows, True)
        hidden, d_act_gate, d_act_up, result, d_expert_in = own_tiles(x, d_rows, w_gate, w_up, w_down, plan)
        half, quarter = own_blocks // 2, own_blocks // 4
        d_away, d_far, d_near = combine(d_expert_in, pos_t, gates_t, None, plan, 0, (half, quarter, quarter), False)
        result, d_away = after(result, d_away)
        d_met = to_core(d_away)
        away, d_gate_away = combine(result, pos_t, gates_t, all_d_out, plan, 0, (half,), True)
        result, (away, d_gate_away, d_far) = after(result, (away, d_gate_away, d_far + d_met[:tok_rows]))
        d_crossed = to_ep(d_far)
        met = to_core(away)
        d_gate_met = to_core(d_gate_away)
        far, near, d_gate_mine = combine(result, pos_t, gates_t, all_d_out, plan, half, (quarter, quarter), True)
        d_gate_mine = d_gate_mine + d_gate_met
        hidden, (far, d_gate_far) = after(hidden, (far + met[:tok_rows], d_gate_mine[:quarter]))
        crossed = to_ep(far)
        d_gate_crossed = to_ep(d_gate_far)
        grads, wholes = [None, None], None
        for part in range(2):
            *grads[part], all_gate, all_up, all_down = rest_tiles(x, d_rows, w_gate, w_up, w_down, hidden, d_act_gate, d_act_up, plan, part, wholes)
            wholes = (all_gate, all_up, all_down)
        d_gates = (d_gate_mine[quarter:] + d_gate_crossed).reshape(tok_rows, top_k)
        d_probs = jnp.sum(jnp.where(expert_hits, d_gates[:, :, None], 0.0), axis=1) + (AUX_COEF * experts / total_tok) * expert_frac[None, :]
        d_logits = (router_probs * (d_probs - jnp.sum(router_probs * d_probs, axis=1, keepdims=True))).astype(jnp.bfloat16)
        grad_router = lax.psum(lax.dot_general(normed, d_logits, TN_DIMS, preferred_element_type=jnp.float32), ("ep", "dp"))
        other_base = (1 - core_at).reshape(1).astype(jnp.int32) * n_exp
        wholes = list(wholes)
        for part in range(2):
            for i in range(3):
                wholes[i] = merge(wholes[i], to_core(grads[part][i]), other_base + part * (n_exp // 2))
        all_gate, all_up, all_down = wholes
        layer_out = (tokens32 + (near + met[tok_rows:] + crossed)).astype(jnp.bfloat16)
        d_normed = (d_near + d_met[tok_rows:] + d_crossed) + lax.dot_general(d_logits, router, NT_DIMS, preferred_element_type=jnp.float32)
        d_tokens = (d_out.astype(jnp.float32) + norm_backward(tokens32, inv_rms, gain32, d_normed)).astype(jnp.bfloat16)
        return layer_out, aux_loss.reshape(1), d_tokens, grad_router, all_gate, all_up, all_down

    return jax.shard_map(device_step, mesh=mesh, in_specs=(tok_spec, tok_spec, tok_spec, P(None), P(None, None), exp_spec, exp_spec, exp_spec), out_specs=(tok_spec, P(None), tok_spec, P(None, None), exp_spec, exp_spec, exp_spec), check_vma=False)
```

```python
import functools

import jax
import jax.numpy as jnp
from jax import lax
from jax.experimental import pallas as pl
from jax.experimental.pallas import tpu as pltpu
from jax.sharding import PartitionSpec as P


AUX_COEF = 0.001
NORM_EPS = 1e-6
MAX_HITS = 416
BLOCK = 256
GROUP = 16
TILE = 512
HALF = TILE // 2
CHUNK = 256
MIX = 256
NT_DIMS = (((1,), (1,)), ((), ()))
TN_DIMS = (((0,), (0,)), ((), ()))
VMEM_LIMIT = 60 * 1024 * 1024


def norm_forward(tokens32, gain32):
    inv_rms = lax.rsqrt(jnp.mean(tokens32 * tokens32, axis=1, keepdims=True) + NORM_EPS)
    return inv_rms, (tokens32 * inv_rms * gain32).astype(jnp.bfloat16)


def norm_backward(tokens32, inv_rms, gain32, d_normed):
    d_scaled = d_normed * gain32
    return inv_rms * (d_scaled - tokens32 * (inv_rms * inv_rms) * jnp.mean(d_scaled * tokens32, axis=1, keepdims=True))


def dot32(left, right, dims=(((1,), (0,)), ((), ()))):
    return lax.dot_general(left, right, dims, preferred_element_type=jnp.float32)


def dispatch_kernel(scaled, begun, first, n_exp, n_chunk, seg_len, seg_src, seg_dst, tail_at, tail_len, pos, gates, *rest):
    *srcs, out, stack, blank, src, sems, src_sems, tail_sem = rest[1:] if begun else rest
    step = pl.program_id(0)
    src_blocks = srcs[0].shape[0] // BLOCK
    last = pl.num_programs(0) - 1
    slot = lax.rem(step, 2)

    def segment_copy(blk, buf, exp, grp):
        at = blk * n_exp + exp
        from_row = pl.multiple_of((seg_src[at] + grp) * GROUP, GROUP)
        to_row = pl.multiple_of((seg_dst[at] + grp) * GROUP, GROUP)
        return pltpu.make_async_copy(stack.at[buf, pl.ds(from_row, GROUP), :], out.at[pl.ds(to_row, GROUP), :], sems.at[buf])

    def each_segment(blk, buf, act):
        for exp in range(n_exp):
            @pl.loop(0, seg_len[blk * n_exp + exp])
            def _(grp):
                act(segment_copy(blk, buf, exp, grp))

    def each_tail(act):
        @pl.loop(0, 2 * n_exp)
        def _(tail):
            @pl.loop(0, tail_len[tail])
            def _(grp):
                to_row = pl.multiple_of((tail_at[tail] + grp) * GROUP, GROUP)
                act(pltpu.make_async_copy(blank, out.at[pl.ds(to_row, GROUP), :], tail_sem))

    def start_source(blk, buf):
        which = lax.div(blk, src_blocks)
        at = pl.ds(pl.multiple_of(lax.rem(blk, src_blocks) * BLOCK, BLOCK), BLOCK)
        for k, ref in enumerate(srcs):
            @pl.when(which == k)
            def _():
                pltpu.make_async_copy(ref.at[at, :], src.at[buf], src_sems.at[buf]).start()

    @pl.when(step == 0)
    def _():
        start_source(step, 0)

    @pl.when(step < last)
    def _():
        start_source(step + 1, 1 - slot)

    pltpu.make_async_copy(srcs[0].at[pl.ds(0, BLOCK), :], src.at[slot], src_sems.at[slot]).wait()

    if not begun:
        @pl.when(step == 0)
        def _():
            blank[...] = jnp.zeros_like(blank)
            each_tail(lambda copy: copy.start())

    @pl.when(step >= 2)
    def _():
        each_segment(first + step - 2, slot, lambda copy: copy.wait())

    @pl.loop(0, n_chunk[first + step])
    def _(chunk):
        row = lax.broadcasted_iota(jnp.int32, (CHUNK, BLOCK), 0) + chunk * CHUNK
        hit = pos[0, 0:1, :] == row
        if scaled:
            weight = jnp.where(hit, gates[0, 0:1, :], 0.0)
        for k in range(1, pos.shape[1]):
            here = pos[0, k:k + 1, :] == row
            hit = jnp.logical_or(hit, here)
            if scaled:
                weight = jnp.where(here, gates[0, k:k + 1, :], weight)
        picked = dot32(jnp.where(hit, 1.0, 0.0).astype(jnp.bfloat16), src[slot])
        if scaled:
            picked = picked * jnp.sum(weight, axis=1, keepdims=True)
        stack[slot, pl.ds(pl.multiple_of(chunk * CHUNK, CHUNK), CHUNK), :] = picked.astype(jnp.bfloat16)

    each_segment(first + step, slot, lambda copy: copy.start())

    @pl.when(step == last)
    def _():
        each_segment(first + step - 1, 1 - slot, lambda copy: copy.wait())
        each_segment(first + step, slot, lambda copy: copy.wait())
        if not begun:
            each_tail(lambda copy: copy.wait())


def dispatch(srcs, pos, gates, plan, first, out, rows, scaled):
    top_k = pos.shape[1]
    begun = out is not None
    width = srcs[0].shape[1]
    n_exp = plan["n_exp"]
    stack_rows = -(-(BLOCK * top_k + n_exp * (GROUP - 1)) // CHUNK) * CHUNK
    any_spec = pl.BlockSpec(memory_space=pl.ANY)
    return pl.pallas_call(
        functools.partial(dispatch_kernel, scaled, begun, first, n_exp),
        out_shape=jax.ShapeDtypeStruct((rows, width), jnp.bfloat16),
        grid_spec=pltpu.PrefetchScalarGridSpec(
            num_scalar_prefetch=6,
            grid=(sum(src.shape[0] for src in srcs) // BLOCK,),
            in_specs=[
                pl.BlockSpec((1, top_k, BLOCK), lambda i, *_: (first + i, 0, 0)),
                pl.BlockSpec((1, top_k, BLOCK), lambda i, *_: (first + i, 0, 0)),
            ]
            + [any_spec] * (begun + len(srcs)),
            out_specs=any_spec,
            scratch_shapes=[
                pltpu.VMEM((2, stack_rows, width), jnp.bfloat16),
                pltpu.VMEM((GROUP, width), jnp.bfloat16),
                pltpu.VMEM((2, BLOCK, width), jnp.bfloat16),
                pltpu.SemaphoreType.DMA((2,)),
                pltpu.SemaphoreType.DMA((2,)),
                pltpu.SemaphoreType.DMA,
            ],
        ),
        compiler_params=pltpu.CompilerParams(dimension_semantics=("arbitrary",), vmem_limit_bytes=VMEM_LIMIT),
        input_output_aliases={8: 0} if begun else {},
        cost_estimate=pl.CostEstimate(flops=40_000_000_000, bytes_accessed=80_000_000, transcendentals=0),
        name="dispatch_scaled" if scaled else "dispatch",
    )(plan["n_chunk"], plan["seg_len"], plan["seg_src"], plan["seg_dst"], plan["tail_at"], plan["tail_len"], pos, gates, *([out] * begun), *srcs)


def combine_kernel(weighted, first, counts, dev_blocks, n_exp, n_mix, seg_len, seg_src, seg_dst, rows, pos, gates, *rest):
    if weighted:
        d_out0, d_out1, *outs, d_gates, stack, total, sems = rest
    else:
        *outs, stack, total, sems = rest
    step = pl.program_id(0)
    blocks = pl.num_programs(0)
    slot = lax.rem(step, 2)

    def each_segment(blk, buf, act):
        for exp in range(n_exp):
            @pl.loop(0, seg_len[blk * n_exp + exp])
            def _(grp):
                at = blk * n_exp + exp
                to_row = pl.multiple_of((seg_src[at] + grp) * GROUP, GROUP)
                from_row = pl.multiple_of((seg_dst[at] + grp) * GROUP, GROUP)
                act(pltpu.make_async_copy(rows.at[pl.ds(from_row, GROUP), :], stack.at[buf, pl.ds(to_row, GROUP), :], sems.at[buf]))

    @pl.when(step == 0)
    def _():
        @pl.loop(0, stack.shape[1] // MIX)
        def _(part):
            stack[:, pl.ds(pl.multiple_of(part * MIX, MIX), MIX), :] = jnp.zeros((2, MIX, stack.shape[2]), stack.dtype)

        each_segment(first, 0, lambda copy: copy.start())

    @pl.when(step < blocks - 1)
    def _():
        each_segment(first + step + 1, 1 - slot, lambda copy: copy.start())

    each_segment(first + step, slot, lambda copy: copy.wait())
    total[...] = jnp.zeros_like(total)
    if weighted:
        d_gates[...] = jnp.zeros_like(d_gates)

    @pl.loop(0, n_mix[first + step])
    def _(part):
        col = lax.broadcasted_iota(jnp.int32, (BLOCK, MIX), 1) + part * MIX
        part_rows = stack[slot, pl.ds(pl.multiple_of(part * MIX, MIX), MIX), :]
        top_k = pos.shape[2]
        if weighted:
            late = step >= dev_blocks
            cross = dot32(jnp.where(late, d_out1[...], d_out0[...]), part_rows, NT_DIMS)
            weight = jnp.zeros((BLOCK, MIX), jnp.float32)
            d_cols = []
            for k in range(top_k):
                here = pos[0, :, k:k + 1] == col
                weight = jnp.where(here, gates[0, :, k:k + 1], weight)
                d_cols.append(jnp.sum(jnp.where(here, cross, 0.0), axis=1, keepdims=True))
            d_gates[0] += jnp.concatenate(d_cols, axis=1)
            high = weight.astype(jnp.bfloat16)
            left = weight - high.astype(jnp.float32)
            mid = left.astype(jnp.bfloat16)
            low = (left - mid.astype(jnp.float32)).astype(jnp.bfloat16)
            mixed = dot32(jnp.concatenate([high, mid, low], axis=0), part_rows)
            total[...] += mixed[:BLOCK] + mixed[BLOCK:2 * BLOCK] + mixed[2 * BLOCK:]
        else:
            hit = pos[0, :, 0:1] == col
            for k in range(1, top_k):
                hit = jnp.logical_or(hit, pos[0, :, k:k + 1] == col)
            total[...] += dot32(jnp.where(hit, 1.0, 0.0).astype(jnp.bfloat16), part_rows)

    begin = 0
    for out, count in zip(outs, counts):
        @pl.when((step >= begin) & (step < begin + count))
        def _():
            out[...] = total[...]

        begin += count


def combine(rows, pos_t, gates_t, d_outs, plan, first, counts, weighted):
    _, _, top_k = pos_t.shape
    width = rows.shape[1]
    n_exp = plan["n_exp"]
    blocks = sum(counts)
    dev_blocks = plan["dev_blocks"]
    stack_rows = -(-(BLOCK * top_k + n_exp * (GROUP - 1)) // MIX) * MIX
    out_shape, out_specs, begin = [], [], 0
    for count in counts:
        out_shape.append(jax.ShapeDtypeStruct((count * BLOCK, width), jnp.float32))
        out_specs.append(pl.BlockSpec((BLOCK, width), lambda i, *_, begin=begin, count=count: (jnp.clip(i - begin, 0, count - 1), 0)))
        begin += count
    d_specs = []
    if weighted:
        out_shape.append(jax.ShapeDtypeStruct((blocks, BLOCK, top_k), jnp.float32))
        out_specs.append(pl.BlockSpec((1, BLOCK, top_k), lambda i, *_: (i, 0, 0)))
        d_specs = [
            pl.BlockSpec((BLOCK, width), lambda i, *_: (jnp.minimum(i, dev_blocks - 1), 0)),
            pl.BlockSpec((BLOCK, width), lambda i, *_: (jnp.maximum(i - dev_blocks, 0), 0)),
        ]
    return pl.pallas_call(
        functools.partial(combine_kernel, weighted, first, counts, dev_blocks, n_exp),
        out_shape=out_shape,
        grid_spec=pltpu.PrefetchScalarGridSpec(
            num_scalar_prefetch=4,
            grid=(blocks,),
            in_specs=[
                pl.BlockSpec(memory_space=pl.ANY),
                pl.BlockSpec((1, BLOCK, top_k), lambda i, *_: (first + i, 0, 0)),
                pl.BlockSpec((1, BLOCK, top_k), lambda i, *_: (first + i, 0, 0)),
            ]
            + d_specs,
            out_specs=out_specs,
            scratch_shapes=[
                pltpu.VMEM((2, stack_rows, width), jnp.bfloat16),
                pltpu.VMEM((BLOCK, width), jnp.float32),
                pltpu.SemaphoreType.DMA((2,)),
            ],
        ),
        compiler_params=pltpu.CompilerParams(dimension_semantics=("arbitrary",), vmem_limit_bytes=VMEM_LIMIT),
        cost_estimate=pl.CostEstimate(flops=5_000_000_000 * blocks, bytes_accessed=60_000_000, transcendentals=0),
        name="combine_weighted" if weighted else "combine",
    )(plan["n_mix"], plan["seg_len"], plan["seg_src"], plan["seg_own"], rows, pos_t, gates_t, *(d_outs if weighted else ()))


def by_kind(kind, body):
    for code, rows in ((1, HALF), (2, TILE)):
        @pl.when(kind == code)
        def _():
            body(pl.ds(0, rows))


def activations(x, w_gate, w_up):
    a = dot32(x, w_gate)
    b = dot32(x, w_up)
    sig = jax.nn.sigmoid(a)
    return a, b, sig, (a * sig * b).astype(jnp.bfloat16)


def cotangents(d_rows, w_down, a, b, sig):
    d_hidden = dot32(d_rows, w_down, NT_DIMS)
    d_a = (d_hidden * b * sig * (1.0 + a * (1.0 - sig))).astype(jnp.bfloat16)
    return d_a, (d_hidden * (a * sig)).astype(jnp.bfloat16)


def own_kernel(tile_exp, tile_at, own_at, tile_kind, x, d_rows, w_gate, w_up, w_down, hidden, d_gate, d_up, result, d_in):
    @pl.loop(0, tile_kind[pl.program_id(0)])
    def _(half):
        part = pl.ds(pl.multiple_of(half * HALF, HALF), HALF)
        a, b, sig, u = activations(x[part], w_gate[0], w_up[0])
        hidden[part] = u
        result[part] = dot32(u, w_down[0]).astype(jnp.bfloat16)
        d_a, d_b = cotangents(d_rows[part], w_down[0], a, b, sig)
        d_gate[part] = d_a
        d_up[part] = d_b
        d_in[part] = (dot32(d_a, w_gate[0], NT_DIMS) + dot32(d_b, w_up[0], NT_DIMS)).astype(jnp.bfloat16)


def rest_kernel(begun, tile_exp, tile_at, own_at, own_kind, other_kind, tile_first, tile_last, base, x, d_rows, w_gate, w_up, w_down, hidden, d_gate, d_up, *refs):
    g_gate, g_up, g_down, all_gate, all_up, all_down, s_gate, s_up, s_down, t_hidden, t_gate, t_up = refs[3:] if begun else refs
    step = pl.program_id(0)

    @pl.when(tile_first[step] > 0)
    def _():
        for total in (s_gate, s_up, s_down):
            total[...] = jnp.zeros_like(total)

    def add(u, d_a, d_b, part):
        s_gate[...] += dot32(x[part], d_a[part], TN_DIMS)
        s_up[...] += dot32(x[part], d_b[part], TN_DIMS)
        s_down[...] += dot32(u[part], d_rows[part], TN_DIMS)

    @pl.loop(0, other_kind[step])
    def _(half):
        part = pl.ds(pl.multiple_of(half * HALF, HALF), HALF)
        a, b, sig, u = activations(x[part], w_gate[0], w_up[0])
        t_hidden[part] = u
        t_gate[part], t_up[part] = cotangents(d_rows[part], w_down[0], a, b, sig)

    by_kind(own_kind[step], functools.partial(add, hidden, d_gate, d_up))
    by_kind(other_kind[step], functools.partial(add, t_hidden, t_gate, t_up))

    @pl.when(tile_last[step] > 0)
    def _():
        for out, whole, total in ((g_gate, all_gate, s_gate), (g_up, all_up, s_up), (g_down, all_down, s_down)):
            rounded = total[...].astype(jnp.bfloat16)
            out[0] = rounded
            whole[0] = rounded


def kernel_params():
    return pltpu.CompilerParams(dimension_semantics=("arbitrary",), vmem_limit_bytes=VMEM_LIMIT)


def own_tiles(x, d_rows, w_gate, w_up, w_down, plan):
    width = x.shape[1]
    mid = w_gate.shape[2]
    wide = pl.BlockSpec((TILE, width), lambda t, exp, at, *_: (at[t], 0))
    thin = pl.BlockSpec((TILE, mid), lambda t, exp, at, own, *_: (own[t], 0))
    wide_own = pl.BlockSpec((TILE, width), lambda t, exp, at, own, *_: (own[t], 0))
    w_in = pl.BlockSpec((1, width, mid), lambda t, exp, *_: (exp[t], 0, 0))
    w_out = pl.BlockSpec((1, mid, width), lambda t, exp, *_: (exp[t], 0, 0))
    seq = plan["own_seq"]
    own_rows = seq[0].shape[0] * TILE
    thin_shape = jax.ShapeDtypeStruct((own_rows, mid), jnp.bfloat16)
    wide_shape = jax.ShapeDtypeStruct((own_rows, width), jnp.bfloat16)
    return pl.pallas_call(
        own_kernel,
        out_shape=[thin_shape] * 3 + [wide_shape] * 2,
        grid_spec=pltpu.PrefetchScalarGridSpec(num_scalar_prefetch=4, grid=(seq[0].shape[0],), in_specs=[wide, wide, w_in, w_in, w_out], out_specs=[thin] * 3 + [wide_own] * 2),
        compiler_params=kernel_params(),
        cost_estimate=pl.CostEstimate(flops=120_000_000_000, bytes_accessed=250_000_000, transcendentals=0),
        name="own_tiles",
    )(*seq, x, d_rows, w_gate, w_up, w_down)


def rest_tiles(x, d_rows, w_gate, w_up, w_down, hidden, d_gate, d_up, plan, half, begun):
    width, mid = w_gate.shape[1:]
    n_half = plan["n_exp"] // 2
    seq = plan["rest_seq"][half]
    shapes = [(width, mid), (width, mid), (mid, width)]
    wide = pl.BlockSpec((TILE, width), lambda t, exp, at, *_: (at[t], 0))
    kept = pl.BlockSpec((TILE, mid), lambda t, exp, at, own, *_: (own[t], 0))
    w_in = pl.BlockSpec((1, width, mid), lambda t, exp, at, own, k1, k2, first, last, base: (base[0] + exp[t], 0, 0))
    w_out = pl.BlockSpec((1, mid, width), lambda t, exp, at, own, k1, k2, first, last, base: (base[0] + exp[t], 0, 0))
    alone = [pl.BlockSpec((1, *shape), lambda t, exp, *_: (exp[t] - half * n_half, 0, 0)) for shape in shapes]
    return pl.pallas_call(
        functools.partial(rest_kernel, begun is not None),
        out_shape=[jax.ShapeDtypeStruct((n_half, *shape), jnp.bfloat16) for shape in shapes]
        + [jax.ShapeDtypeStruct((4 * n_half, *shape), jnp.bfloat16) for shape in shapes],
        grid_spec=pltpu.PrefetchScalarGridSpec(
            num_scalar_prefetch=8,
            grid=(seq[0].shape[0],),
            in_specs=[wide, wide, w_in, w_in, w_out, kept, kept, kept] + [pl.BlockSpec(memory_space=pl.ANY)] * (3 if begun else 0),
            out_specs=alone + [w_in, w_in, w_out],
            scratch_shapes=[pltpu.VMEM(shape, jnp.float32) for shape in shapes] + [pltpu.VMEM((TILE, mid), jnp.bfloat16)] * 3,
        ),
        input_output_aliases={16: 3, 17: 4, 18: 5} if begun else {},
        compiler_params=kernel_params(),
        cost_estimate=pl.CostEstimate(flops=80_000_000_000, bytes_accessed=150_000_000, transcendentals=0),
        name="rest_tiles",
    )(*seq, plan["base"], x, d_rows, w_gate, w_up, w_down, hidden, d_gate, d_up, *(begun or ()))


def merge_kernel(base, whole_in, other, whole):
    whole[...] = other[...]


def merge(whole, other, other_base):
    count, *shape = other.shape
    return pl.pallas_call(
        merge_kernel,
        out_shape=jax.ShapeDtypeStruct(whole.shape, whole.dtype),
        grid_spec=pltpu.PrefetchScalarGridSpec(
            num_scalar_prefetch=1,
            grid=(count,),
            in_specs=[pl.BlockSpec(memory_space=pl.ANY), pl.BlockSpec((1, *shape), lambda i, base: (i, 0, 0))],
            out_specs=pl.BlockSpec((1, *shape), lambda i, base: (base[0] + i, 0, 0)),
        ),
        input_output_aliases={1: 0},
        compiler_params=pltpu.CompilerParams(dimension_semantics=("arbitrary",), vmem_limit_bytes=16 * 1024 * 1024),
        cost_estimate=pl.CostEstimate(flops=8_000_000_000, bytes_accessed=30_000_000, transcendentals=0),
        name="merge",
    )(other_base, whole, other)


def exclusive(values, axis=0):
    return jnp.cumsum(values, axis=axis) - values


def make_plan(local_ids, own_blocks, n_exp, max_tiles, max_own, weight_base):
    onehot = (local_ids[:, :, None, :] == jnp.arange(n_exp)[None, None, :, None]).astype(jnp.float32)
    hits = jnp.sum(onehot, axis=1)
    before = jnp.triu(jnp.ones((BLOCK, BLOCK), jnp.bfloat16), 1)
    rank = jnp.einsum("oet,ts->oes", hits.astype(jnp.bfloat16), before, preferred_element_type=jnp.float32)
    seg_len = (jnp.sum(hits, axis=2).astype(jnp.int32) + GROUP - 1) // GROUP
    seg_src = exclusive(seg_len, 1)
    per_tile, per_half = TILE // GROUP, HALF // GROUP
    groups = jnp.stack([jnp.sum(seg_len[:own_blocks], axis=0), jnp.sum(seg_len[own_blocks:], axis=0)])
    both_tiles = (groups + per_tile - 1) // per_tile
    own_tiles, other_tiles = both_tiles
    tiles = own_tiles + other_tiles
    tile_base = exclusive(tiles)
    begins = jnp.stack([tile_base, tile_base + own_tiles]) * per_tile
    seg_dst = jnp.concatenate([begins[0] + exclusive(seg_len[:own_blocks], 0), begins[1] + exclusive(seg_len[own_blocks:], 0)])
    place = rank + (seg_src * GROUP).astype(jnp.float32)[:, :, None]
    pos = jnp.sum(onehot * (place[:, None] + 1.0), axis=2).astype(jnp.int32) - 1
    exp_ids = jnp.arange(n_exp)

    def sequence(counts, length):
        ids = jnp.arange(length)
        at = jnp.minimum(ids, jnp.maximum(jnp.sum(counts) - 1, 0))
        ends = jnp.cumsum(counts)
        exp = jnp.minimum(jnp.sum((at[:, None] >= ends[None, :]).astype(jnp.int32), axis=1), n_exp - 1)
        is_exp = (exp[:, None] == exp_ids[None, :]).astype(jnp.int32)
        pick = lambda table: jnp.sum(is_exp * table[None, :], axis=1)
        return exp, at - pick(ends - counts), ids > at, pick

    def kind_of(left, past):
        return jnp.where(past, 0, jnp.where(left <= per_half, 1, 2))

    o_exp, o_nth, o_past, o_pick = sequence(own_tiles, max_own)
    own_base = exclusive(own_tiles)

    def rest_seq(half):
        mine = exp_ids // (n_exp // 2) == half
        exp, nth, past, pick = sequence(jnp.where(mine, tiles, 0), max_tiles // 2)
        own_count = pick(own_tiles)
        is_own = nth < own_count
        kind = kind_of(jnp.where(is_own, pick(groups[0]) - nth * per_tile, pick(groups[1]) - (nth - own_count) * per_tile), past)
        seq = (
            exp,
            pick(tile_base) + nth,
            pick(own_base) + jnp.minimum(nth, own_count - 1),
            jnp.where(is_own, kind, 0),
            jnp.where(is_own, 0, kind),
            (nth == 0) & ~past,
            (nth == pick(tiles) - 1) & ~past,
        )
        return seq

    stack_rows = jnp.sum(seg_len, axis=1) * GROUP
    plan = {
        "n_chunk": (stack_rows + CHUNK - 1) // CHUNK,
        "n_mix": (stack_rows + MIX - 1) // MIX,
        "seg_len": seg_len.reshape(-1),
        "seg_src": seg_src.reshape(-1),
        "seg_dst": seg_dst.reshape(-1),
        "seg_own": (own_base[None, :] * per_tile + exclusive(seg_len, 0)).reshape(-1),
        "tail_at": (begins + groups).reshape(-1),
        "tail_len": ((groups + per_half - 1) // per_half * per_half - groups).reshape(-1),
        "base": weight_base.reshape(1),
        "own_seq": (o_exp + weight_base, o_pick(tile_base) + o_nth, o_pick(own_base) + o_nth, kind_of(o_pick(groups[0]) - o_nth * per_tile, o_past)),
        "rest_seq": (rest_seq(0), rest_seq(1)),
    }
    return jax.tree.map(lambda value: value.astype(jnp.int32), plan), pos


def solution(mesh):
    ep_size = mesh.shape["ep"]
    dp_size = mesh.shape["dp"]
    devices = ep_size * dp_size
    cores = 2
    tok_spec = P(("dp", "ep"), None)
    exp_spec = P("ep", None, None)
    core_perm = [(i, i ^ 1) for i in range(dp_size)]
    x_perm = [(i, i ^ cores) for i in range(dp_size)]
    ep_perm = [(i, i ^ 1) for i in range(ep_size)]

    def to_core(away):
        return lax.ppermute(away, "dp", core_perm)

    def to_ep(far):
        return lax.ppermute(far, "ep", ep_perm)

    def to_x(block):
        return lax.ppermute(block, "dp", x_perm)

    def spread(block):
        ep_block = to_ep(block)
        core_block = to_core(block)
        own = (to_core(ep_block), core_block, ep_block, block)
        return own, (to_x(block), to_x(ep_block))

    def after(value, other):
        return lax.optimization_barrier((value, other))

    def device_step(tokens, d_out, expert_ids, norm_gain, router, w_gate, w_up, w_down):
        tok_rows, _ = tokens.shape
        top_k = expert_ids.shape[1]
        local_experts = w_gate.shape[0]
        experts = local_experts * ep_size
        total_tok = tok_rows * devices
        n_exp = local_experts // cores
        dev_blocks = tok_rows // BLOCK
        own_devs = devices // 2
        own_blocks = own_devs * dev_blocks
        max_own = n_exp * -(-(own_devs * MAX_HITS + own_blocks * (GROUP - 1)) // TILE)
        max_tiles = 2 * max_own

        ep_at = lax.axis_index("ep")
        dp_at = lax.axis_index("dp")
        core_at = lax.rem(dp_at, cores)
        x_at = lax.div(dp_at, cores)

        def dev_of(x, core, ep):
            return (x * cores + core) * ep_size + ep

        dev_order = jnp.stack(
            [dev_of(x_at, 1 - core_at, 1 - ep_at), dev_of(x_at, 1 - core_at, ep_at), dev_of(x_at, core_at, 1 - ep_at), dev_of(x_at, core_at, ep_at)]
            + [dev_of(1 - x_at, core_at, ep_at), dev_of(1 - x_at, core_at, 1 - ep_at), dev_of(1 - x_at, 1 - core_at, ep_at), dev_of(1 - x_at, 1 - core_at, 1 - ep_at)]
        )
        tokens32 = tokens.astype(jnp.float32)
        gain32 = norm_gain.astype(jnp.float32)
        inv_rms, normed = norm_forward(tokens32, gain32)
        logits = jnp.dot(normed, router, preferred_element_type=jnp.float32)
        router_probs = jax.nn.softmax(logits, axis=1)
        expert_hits = expert_ids[:, :, None] == jnp.arange(experts)[None, None, :]
        gate_vals = jnp.sum(jnp.where(expert_hits, router_probs[:, None, :], 0.0), axis=2)

        prob_sums = jnp.pad(jnp.sum(router_probs, axis=0), (0, tok_rows - experts))
        packet = jnp.concatenate([expert_ids.astype(jnp.float32).T, gate_vals.T, prob_sums[None]], axis=0)
        packets = lax.all_gather(packet, ("dp", "ep"))
        own_d_out, x_d_out = spread(d_out)
        own_normed, x_normed = spread(normed)

        all_ids = packets[:, :top_k].astype(jnp.int32)
        counts = jnp.sum((all_ids[..., None] == jnp.arange(experts)).astype(jnp.float32), axis=(0, 1, 2))
        expert_frac = counts / (total_tok * top_k)
        aux_loss = AUX_COEF * experts * jnp.sum(expert_frac * jnp.sum(packets[:, 2 * top_k, :experts], axis=0)) / total_tok

        turned = jnp.take(packets, dev_order, axis=0)

        def by_block(rows):
            return rows.reshape(devices, top_k, dev_blocks, BLOCK).transpose(0, 2, 1, 3).reshape(devices * dev_blocks, top_k, BLOCK)

        first_expert = ep_at * local_experts + core_at * n_exp
        block_ids = by_block(turned[:, :top_k]).astype(jnp.int32) - first_expert
        block_ids = jnp.where((block_ids >= 0) & (block_ids < n_exp), block_ids, n_exp)
        block_gates = by_block(turned[:, top_k:2 * top_k])
        plan, pos = make_plan(block_ids, own_blocks, n_exp, max_tiles, max_own, core_at * n_exp)
        plan.update(dev_blocks=dev_blocks, n_exp=n_exp)
        pos_t = pos[:own_blocks].transpose(0, 2, 1)
        gates_t = block_gates[:own_blocks].transpose(0, 2, 1)

        rows = max_tiles * TILE
        d_rows = dispatch(own_d_out, pos, block_gates, plan, 0, None, rows, True)
        x = dispatch(own_normed, pos, block_gates, plan, 0, None, rows, False)
        hidden, d_act_gate, d_act_up, result, d_expert_in = own_tiles(x, d_rows, w_gate, w_up, w_down, plan)
        d_rows, result = after(d_rows, result)
        x_d_out, result = after(x_d_out, result)
        x_normed, result = after(x_normed, result)
        x_d_out = (*x_d_out, *(to_core(block) for block in x_d_out))
        x_normed = (*x_normed, *(to_core(block) for block in x_normed))
        half, quarter = own_blocks // 2, own_blocks // 4
        d_away, d_far, d_near = combine(d_expert_in, pos_t, gates_t, None, plan, 0, (half, quarter, quarter), False)
        result, d_away = after(result, d_away)
        d_met = to_core(d_away)
        away, d_gate_away = combine(result, pos_t, gates_t, own_d_out[:2], plan, 0, (half,), True)
        result, (away, d_gate_away, d_far) = after(result, (away, d_gate_away, d_far + d_met[:tok_rows]))
        d_crossed = to_ep(d_far)
        met = to_core(away)
        d_gate_met = to_core(d_gate_away)
        far, near, d_gate_mine = combine(result, pos_t, gates_t, own_d_out[2:], plan, half, (quarter, quarter), True)
        d_gate_mine = d_gate_mine + d_gate_met
        hidden, (far, d_gate_far) = after(hidden, (far + met[:tok_rows], d_gate_mine[:quarter]))
        crossed = to_ep(far)
        d_gate_crossed = to_ep(d_gate_far)
        d_rows, hidden = after(d_rows, hidden)
        d_rows = dispatch(x_d_out, pos, block_gates, plan, own_blocks, d_rows, rows, True)
        x = dispatch(x_normed, pos, block_gates, plan, own_blocks, x, rows, False)
        grads, wholes = [None, None], None
        for part in range(2):
            *grads[part], all_gate, all_up, all_down = rest_tiles(x, d_rows, w_gate, w_up, w_down, hidden, d_act_gate, d_act_up, plan, part, wholes)
            wholes = (all_gate, all_up, all_down)
        d_gates = (d_gate_mine[quarter:] + d_gate_crossed).reshape(tok_rows, top_k)
        d_probs = jnp.sum(jnp.where(expert_hits, d_gates[:, :, None], 0.0), axis=1) + (AUX_COEF * experts / total_tok) * expert_frac[None, :]
        d_logits = (router_probs * (d_probs - jnp.sum(router_probs * d_probs, axis=1, keepdims=True))).astype(jnp.bfloat16)
        grad_router = lax.psum(lax.dot_general(normed, d_logits, TN_DIMS, preferred_element_type=jnp.float32), ("ep", "dp"))
        other_base = (1 - core_at).reshape(1).astype(jnp.int32) * n_exp
        wholes = list(wholes)
        for part in range(2):
            for i in range(3):
                wholes[i] = merge(wholes[i], to_core(grads[part][i]), other_base + part * (n_exp // 2))
        all_gate, all_up, all_down = wholes
        layer_out = (tokens32 + (near + met[tok_rows:] + crossed)).astype(jnp.bfloat16)
        d_normed = (d_near + d_met[tok_rows:] + d_crossed) + lax.dot_general(d_logits, router, NT_DIMS, preferred_element_type=jnp.float32)
        d_tokens = (d_out.astype(jnp.float32) + norm_backward(tokens32, inv_rms, gain32, d_normed)).astype(jnp.bfloat16)
        return layer_out, aux_loss.reshape(1), d_tokens, grad_router, all_gate, all_up, all_down

    return jax.shard_map(device_step, mesh=mesh, in_specs=(tok_spec, tok_spec, tok_spec, P(None), P(None, None), exp_spec, exp_spec, exp_spec), out_specs=(tok_spec, P(None), tok_spec, P(None, None), exp_spec, exp_spec, exp_spec), check_vma=False)
```

```python
import functools
from typing import Any, NamedTuple

import jax
import jax.numpy as jnp
from jax import lax
from jax.experimental import pallas as pl
from jax.experimental.pallas import tpu as pltpu
from jax.sharding import PartitionSpec as P


AUX_COEF = 0.001
NORM_EPS = 1e-6
MAX_HITS = 416
BLOCK = 256
GROUP = 16
TILE = 512
HALF = TILE // 2
CHUNK = 256
MIX = 256
NT_DIMS = (((1,), (1,)), ((), ()))
TN_DIMS = (((0,), (0,)), ((), ()))
VMEM_LIMIT = 60 * 1024 * 1024


def norm_forward(tokens32, gain32):
    inv_rms = lax.rsqrt(jnp.mean(tokens32 * tokens32, axis=1, keepdims=True) + NORM_EPS)
    return inv_rms, (tokens32 * inv_rms * gain32).astype(jnp.bfloat16)


def norm_backward(tokens32, inv_rms, gain32, d_normed):
    d_scaled = d_normed * gain32
    return inv_rms * (d_scaled - tokens32 * (inv_rms * inv_rms) * jnp.mean(d_scaled * tokens32, axis=1, keepdims=True))


def dot32(left, right, dims=(((1,), (0,)), ((), ()))):
    return lax.dot_general(left, right, dims, preferred_element_type=jnp.float32)


def sized_copies(groups, copy):
    fours = lax.div(groups, 4)

    @pl.loop(0, fours)
    def _(i):
        copy(4 * i, 4)

    left = groups - 4 * fours

    @pl.when(left >= 2)
    def _():
        copy(4 * fours, 2)

    @pl.when(lax.rem(left, 2) == 1)
    def _():
        copy(groups - 1, 1)


def dispatch_kernel(scaled, begun, first, n_exp, n_chunk, n_group, seg_len, seg_src, seg_dst, tail_at, tail_len, pos, gates, *rest):
    *srcs, out, stack, blank, src, sems, src_sems, tail_sem = rest[1:] if begun else rest
    step = pl.program_id(0)
    src_blocks = srcs[0].shape[0] // BLOCK
    last = pl.num_programs(0) - 1
    slot = lax.rem(step, 2)

    def send_segments(blk, buf):
        @pl.loop(0, n_exp)
        def _(exp):
            at = blk * n_exp + exp

            def send(grp, count):
                from_row = pl.multiple_of((seg_src[at] + grp) * GROUP, GROUP)
                to_row = pl.multiple_of((seg_dst[at] + grp) * GROUP, GROUP)
                pltpu.make_async_copy(stack.at[buf, pl.ds(from_row, count * GROUP), :], out.at[pl.ds(to_row, count * GROUP), :], sems.at[buf]).start()

            sized_copies(seg_len[at], send)

    def await_segments(blk, buf):
        def wait(grp, count):
            pltpu.make_async_copy(stack.at[buf, pl.ds(0, count * GROUP), :], out.at[pl.ds(0, count * GROUP), :], sems.at[buf]).wait()

        sized_copies(n_group[blk], wait)

    def each_tail(act):
        @pl.loop(0, 2 * n_exp)
        def _(tail):
            @pl.loop(0, tail_len[tail])
            def _(grp):
                to_row = pl.multiple_of((tail_at[tail] + grp) * GROUP, GROUP)
                act(pltpu.make_async_copy(blank, out.at[pl.ds(to_row, GROUP), :], tail_sem))

    def start_source(blk, buf):
        which = lax.div(blk, src_blocks)
        at = pl.ds(pl.multiple_of(lax.rem(blk, src_blocks) * BLOCK, BLOCK), BLOCK)
        for k, ref in enumerate(srcs):
            @pl.when(which == k)
            def _():
                pltpu.make_async_copy(ref.at[at, :], src.at[buf], src_sems.at[buf]).start()

    @pl.when(step == 0)
    def _():
        start_source(step, 0)

    @pl.when(step < last)
    def _():
        start_source(step + 1, 1 - slot)

    pltpu.make_async_copy(srcs[0].at[pl.ds(0, BLOCK), :], src.at[slot], src_sems.at[slot]).wait()

    if not begun:
        @pl.when(step == 0)
        def _():
            blank[...] = jnp.zeros_like(blank)
            each_tail(lambda copy: copy.start())

    @pl.when(step >= 2)
    def _():
        await_segments(first + step - 2, slot)

    @pl.loop(0, n_chunk[first + step])
    def _(chunk):
        row = lax.broadcasted_iota(jnp.int32, (CHUNK, BLOCK), 0) + chunk * CHUNK
        hit = pos[0, 0:1, :] == row
        if scaled:
            weight = jnp.where(hit, gates[0, 0:1, :], 0.0)
        for k in range(1, pos.shape[1]):
            here = pos[0, k:k + 1, :] == row
            hit = jnp.logical_or(hit, here)
            if scaled:
                weight = jnp.where(here, gates[0, k:k + 1, :], weight)
        picked = dot32(jnp.where(hit, 1.0, 0.0).astype(jnp.bfloat16), src[slot])
        if scaled:
            picked = picked * jnp.sum(weight, axis=1, keepdims=True)
        stack[slot, pl.ds(pl.multiple_of(chunk * CHUNK, CHUNK), CHUNK), :] = picked.astype(jnp.bfloat16)

    send_segments(first + step, slot)

    @pl.when(step == last)
    def _():
        await_segments(first + step - 1, 1 - slot)
        await_segments(first + step, slot)
        if not begun:
            each_tail(lambda copy: copy.wait())


def dispatch(srcs, pos, gates, plan, first, out, rows, scaled):
    top_k = pos.shape[1]
    begun = out is not None
    width = srcs[0].shape[1]
    n_exp = plan.n_exp
    stack_rows = -(-(BLOCK * top_k + n_exp * (GROUP - 1)) // CHUNK) * CHUNK
    any_spec = pl.BlockSpec(memory_space=pl.ANY)
    return pl.pallas_call(
        functools.partial(dispatch_kernel, scaled, begun, first, n_exp),
        out_shape=jax.ShapeDtypeStruct((rows, width), jnp.bfloat16),
        grid_spec=pltpu.PrefetchScalarGridSpec(
            num_scalar_prefetch=7,
            grid=(sum(src.shape[0] for src in srcs) // BLOCK,),
            in_specs=[
                pl.BlockSpec((1, top_k, BLOCK), lambda i, *_: (first + i, 0, 0)),
                pl.BlockSpec((1, top_k, BLOCK), lambda i, *_: (first + i, 0, 0)),
            ]
            + [any_spec] * (begun + len(srcs)),
            out_specs=any_spec,
            scratch_shapes=[
                pltpu.VMEM((2, stack_rows, width), jnp.bfloat16),
                pltpu.VMEM((GROUP, width), jnp.bfloat16),
                pltpu.VMEM((2, BLOCK, width), jnp.bfloat16),
                pltpu.SemaphoreType.DMA((2,)),
                pltpu.SemaphoreType.DMA((2,)),
                pltpu.SemaphoreType.DMA,
            ],
        ),
        compiler_params=pltpu.CompilerParams(dimension_semantics=("arbitrary",), vmem_limit_bytes=VMEM_LIMIT),
        input_output_aliases={9: 0} if begun else {},
        cost_estimate=pl.CostEstimate(flops=40_000_000_000, bytes_accessed=80_000_000, transcendentals=0),
        name="dispatch_scaled" if scaled else "dispatch",
    )(plan.n_chunk, plan.n_group, plan.seg_len, plan.seg_src, plan.seg_dst, plan.tail_at, plan.tail_len, pos, gates, *([out] * begun), *srcs)


def combine_kernel(weighted, first, counts, dev_blocks, n_exp, n_mix, n_group, seg_len, seg_src, seg_dst, rows, pos, gates, *rest):
    if weighted:
        d_out0, d_out1, *outs, d_gates, stack, total, sems = rest
    else:
        *outs, stack, total, sems = rest
    step = pl.program_id(0)
    blocks = pl.num_programs(0)
    slot = lax.rem(step, 2)

    def fetch_segments(blk, buf):
        @pl.loop(0, n_exp)
        def _(exp):
            at = blk * n_exp + exp

            def fetch(grp, count):
                to_row = pl.multiple_of((seg_src[at] + grp) * GROUP, GROUP)
                from_row = pl.multiple_of((seg_dst[at] + grp) * GROUP, GROUP)
                pltpu.make_async_copy(rows.at[pl.ds(from_row, count * GROUP), :], stack.at[buf, pl.ds(to_row, count * GROUP), :], sems.at[buf]).start()

            sized_copies(seg_len[at], fetch)

    def await_segments(blk, buf):
        def wait(grp, count):
            pltpu.make_async_copy(rows.at[pl.ds(0, count * GROUP), :], stack.at[buf, pl.ds(0, count * GROUP), :], sems.at[buf]).wait()

        sized_copies(n_group[blk], wait)

    @pl.when(step == 0)
    def _():
        @pl.loop(0, stack.shape[1] // MIX)
        def _(part):
            stack[:, pl.ds(pl.multiple_of(part * MIX, MIX), MIX), :] = jnp.zeros((2, MIX, stack.shape[2]), stack.dtype)

        fetch_segments(first, 0)

    @pl.when(step < blocks - 1)
    def _():
        fetch_segments(first + step + 1, 1 - slot)

    await_segments(first + step, slot)
    total[...] = jnp.zeros_like(total)
    if weighted:
        d_gates[...] = jnp.zeros_like(d_gates)

    @pl.loop(0, n_mix[first + step])
    def _(part):
        col = lax.broadcasted_iota(jnp.int32, (BLOCK, MIX), 1) + part * MIX
        part_rows = stack[slot, pl.ds(pl.multiple_of(part * MIX, MIX), MIX), :]
        top_k = pos.shape[2]
        if weighted:
            late = step >= dev_blocks
            cross = dot32(jnp.where(late, d_out1[...], d_out0[...]), part_rows, NT_DIMS)
            weight = jnp.zeros((BLOCK, MIX), jnp.float32)
            d_cols = []
            for k in range(top_k):
                here = pos[0, :, k:k + 1] == col
                weight = jnp.where(here, gates[0, :, k:k + 1], weight)
                d_cols.append(jnp.sum(jnp.where(here, cross, 0.0), axis=1, keepdims=True))
            d_gates[0] += jnp.concatenate(d_cols, axis=1)
            high = weight.astype(jnp.bfloat16)
            left = weight - high.astype(jnp.float32)
            mid = left.astype(jnp.bfloat16)
            low = (left - mid.astype(jnp.float32)).astype(jnp.bfloat16)
            mixed = dot32(jnp.concatenate([high, mid, low], axis=0), part_rows)
            total[...] += mixed[:BLOCK] + mixed[BLOCK:2 * BLOCK] + mixed[2 * BLOCK:]
        else:
            hit = pos[0, :, 0:1] == col
            for k in range(1, top_k):
                hit = jnp.logical_or(hit, pos[0, :, k:k + 1] == col)
            total[...] += dot32(jnp.where(hit, 1.0, 0.0).astype(jnp.bfloat16), part_rows)

    begin = 0
    for out, count in zip(outs, counts):
        @pl.when((step >= begin) & (step < begin + count))
        def _():
            out[...] = total[...]

        begin += count


def combine(rows, pos_t, gates_t, d_outs, plan, first, counts, weighted):
    _, _, top_k = pos_t.shape
    width = rows.shape[1]
    n_exp = plan.n_exp
    blocks = sum(counts)
    dev_blocks = plan.dev_blocks
    stack_rows = -(-(BLOCK * top_k + n_exp * (GROUP - 1)) // MIX) * MIX
    out_shape, out_specs, begin = [], [], 0
    for count in counts:
        out_shape.append(jax.ShapeDtypeStruct((count * BLOCK, width), jnp.float32))
        out_specs.append(pl.BlockSpec((BLOCK, width), lambda i, *_, begin=begin, count=count: (jnp.clip(i - begin, 0, count - 1), 0)))
        begin += count
    d_specs = []
    if weighted:
        out_shape.append(jax.ShapeDtypeStruct((blocks, BLOCK, top_k), jnp.float32))
        out_specs.append(pl.BlockSpec((1, BLOCK, top_k), lambda i, *_: (i, 0, 0)))
        d_specs = [
            pl.BlockSpec((BLOCK, width), lambda i, *_: (jnp.minimum(i, dev_blocks - 1), 0)),
            pl.BlockSpec((BLOCK, width), lambda i, *_: (jnp.maximum(i - dev_blocks, 0), 0)),
        ]
    return pl.pallas_call(
        functools.partial(combine_kernel, weighted, first, counts, dev_blocks, n_exp),
        out_shape=out_shape,
        grid_spec=pltpu.PrefetchScalarGridSpec(
            num_scalar_prefetch=5,
            grid=(blocks,),
            in_specs=[
                pl.BlockSpec(memory_space=pl.ANY),
                pl.BlockSpec((1, BLOCK, top_k), lambda i, *_: (first + i, 0, 0)),
                pl.BlockSpec((1, BLOCK, top_k), lambda i, *_: (first + i, 0, 0)),
            ]
            + d_specs,
            out_specs=out_specs,
            scratch_shapes=[
                pltpu.VMEM((2, stack_rows, width), jnp.bfloat16),
                pltpu.VMEM((BLOCK, width), jnp.float32),
                pltpu.SemaphoreType.DMA((2,)),
            ],
        ),
        compiler_params=pltpu.CompilerParams(dimension_semantics=("arbitrary",), vmem_limit_bytes=VMEM_LIMIT),
        cost_estimate=pl.CostEstimate(flops=5_000_000_000 * blocks, bytes_accessed=60_000_000, transcendentals=0),
        name="combine_weighted" if weighted else "combine",
    )(plan.n_mix, plan.n_group, plan.seg_len, plan.seg_src, plan.seg_own, rows, pos_t, gates_t, *(d_outs if weighted else ()))


def by_kind(kind, body):
    for code, rows in ((1, HALF), (2, TILE)):
        @pl.when(kind == code)
        def _():
            body(pl.ds(0, rows))


def activations(x, w_gate, w_up):
    a = dot32(x, w_gate)
    b = dot32(x, w_up)
    sig = jax.nn.sigmoid(a)
    return a, b, sig, (a * sig * b).astype(jnp.bfloat16)


def cotangents(d_rows, w_down, a, b, sig):
    d_hidden = dot32(d_rows, w_down, NT_DIMS)
    d_a = (d_hidden * b * sig * (1.0 + a * (1.0 - sig))).astype(jnp.bfloat16)
    return d_a, (d_hidden * (a * sig)).astype(jnp.bfloat16)


def own_kernel(tile_exp, tile_at, own_at, tile_kind, x, d_rows, w_gate, w_up, w_down, hidden, d_gate, d_up, result, d_in):
    @pl.loop(0, tile_kind[pl.program_id(0)])
    def _(half):
        part = pl.ds(pl.multiple_of(half * HALF, HALF), HALF)
        a, b, sig, u = activations(x[part], w_gate[0], w_up[0])
        hidden[part] = u
        result[part] = dot32(u, w_down[0]).astype(jnp.bfloat16)
        d_a, d_b = cotangents(d_rows[part], w_down[0], a, b, sig)
        d_gate[part] = d_a
        d_up[part] = d_b
        d_in[part] = (dot32(d_a, w_gate[0], NT_DIMS) + dot32(d_b, w_up[0], NT_DIMS)).astype(jnp.bfloat16)


def rest_kernel(begun, tile_exp, tile_at, own_at, own_kind, other_kind, tile_first, tile_last, base, x, d_rows, w_gate, w_up, w_down, hidden, d_gate, d_up, *refs):
    g_gate, g_up, g_down, all_gate, all_up, all_down, s_gate, s_up, s_down, t_hidden, t_gate, t_up = refs[3:] if begun else refs
    step = pl.program_id(0)

    @pl.when(tile_first[step] > 0)
    def _():
        for total in (s_gate, s_up, s_down):
            total[...] = jnp.zeros_like(total)

    def add(u, d_a, d_b, part):
        s_gate[...] += dot32(x[part], d_a[part], TN_DIMS)
        s_up[...] += dot32(x[part], d_b[part], TN_DIMS)
        s_down[...] += dot32(u[part], d_rows[part], TN_DIMS)

    @pl.loop(0, other_kind[step])
    def _(half):
        part = pl.ds(pl.multiple_of(half * HALF, HALF), HALF)
        a, b, sig, u = activations(x[part], w_gate[0], w_up[0])
        t_hidden[part] = u
        t_gate[part], t_up[part] = cotangents(d_rows[part], w_down[0], a, b, sig)

    by_kind(own_kind[step], functools.partial(add, hidden, d_gate, d_up))
    by_kind(other_kind[step], functools.partial(add, t_hidden, t_gate, t_up))

    @pl.when(tile_last[step] > 0)
    def _():
        for out, whole, total in ((g_gate, all_gate, s_gate), (g_up, all_up, s_up), (g_down, all_down, s_down)):
            rounded = total[...].astype(jnp.bfloat16)
            out[0] = rounded
            whole[0] = rounded


def kernel_params():
    return pltpu.CompilerParams(dimension_semantics=("arbitrary",), vmem_limit_bytes=VMEM_LIMIT)


def own_tiles(x, d_rows, w_gate, w_up, w_down, plan):
    width = x.shape[1]
    mid = w_gate.shape[2]
    wide = pl.BlockSpec((TILE, width), lambda t, exp, at, *_: (at[t], 0))
    thin = pl.BlockSpec((TILE, mid), lambda t, exp, at, own, *_: (own[t], 0))
    wide_own = pl.BlockSpec((TILE, width), lambda t, exp, at, own, *_: (own[t], 0))
    w_in = pl.BlockSpec((1, width, mid), lambda t, exp, *_: (exp[t], 0, 0))
    w_out = pl.BlockSpec((1, mid, width), lambda t, exp, *_: (exp[t], 0, 0))
    seq = plan.own_seq
    own_rows = seq[0].shape[0] * TILE
    thin_shape = jax.ShapeDtypeStruct((own_rows, mid), jnp.bfloat16)
    wide_shape = jax.ShapeDtypeStruct((own_rows, width), jnp.bfloat16)
    return pl.pallas_call(
        own_kernel,
        out_shape=[thin_shape] * 3 + [wide_shape] * 2,
        grid_spec=pltpu.PrefetchScalarGridSpec(num_scalar_prefetch=4, grid=(seq[0].shape[0],), in_specs=[wide, wide, w_in, w_in, w_out], out_specs=[thin] * 3 + [wide_own] * 2),
        compiler_params=kernel_params(),
        cost_estimate=pl.CostEstimate(flops=120_000_000_000, bytes_accessed=250_000_000, transcendentals=0),
        name="own_tiles",
    )(*seq, x, d_rows, w_gate, w_up, w_down)


def rest_tiles(x, d_rows, w_gate, w_up, w_down, hidden, d_gate, d_up, plan, half, begun):
    width, mid = w_gate.shape[1:]
    n_half = plan.n_exp // 2
    seq = plan.rest_seq[half]
    shapes = [(width, mid), (width, mid), (mid, width)]
    wide = pl.BlockSpec((TILE, width), lambda t, exp, at, *_: (at[t], 0))
    kept = pl.BlockSpec((TILE, mid), lambda t, exp, at, own, *_: (own[t], 0))
    w_in = pl.BlockSpec((1, width, mid), lambda t, exp, at, own, k1, k2, first, last, base: (base[0] + exp[t], 0, 0))
    w_out = pl.BlockSpec((1, mid, width), lambda t, exp, at, own, k1, k2, first, last, base: (base[0] + exp[t], 0, 0))
    alone = [pl.BlockSpec((1, *shape), lambda t, exp, *_: (exp[t] - half * n_half, 0, 0)) for shape in shapes]
    return pl.pallas_call(
        functools.partial(rest_kernel, begun is not None),
        out_shape=[jax.ShapeDtypeStruct((n_half, *shape), jnp.bfloat16) for shape in shapes]
        + [jax.ShapeDtypeStruct((4 * n_half, *shape), jnp.bfloat16) for shape in shapes],
        grid_spec=pltpu.PrefetchScalarGridSpec(
            num_scalar_prefetch=8,
            grid=(seq[0].shape[0],),
            in_specs=[wide, wide, w_in, w_in, w_out, kept, kept, kept] + [pl.BlockSpec(memory_space=pl.ANY)] * (3 if begun else 0),
            out_specs=alone + [w_in, w_in, w_out],
            scratch_shapes=[pltpu.VMEM(shape, jnp.float32) for shape in shapes] + [pltpu.VMEM((TILE, mid), jnp.bfloat16)] * 3,
        ),
        input_output_aliases={16: 3, 17: 4, 18: 5} if begun else {},
        compiler_params=kernel_params(),
        cost_estimate=pl.CostEstimate(flops=80_000_000_000, bytes_accessed=150_000_000, transcendentals=0),
        name="rest_tiles",
    )(*seq, plan.base, x, d_rows, w_gate, w_up, w_down, hidden, d_gate, d_up, *(begun or ()))


def merge_kernel(base, whole_in, other, whole):
    whole[...] = other[...]


def merge(whole, other, other_base):
    count, *shape = other.shape
    return pl.pallas_call(
        merge_kernel,
        out_shape=jax.ShapeDtypeStruct(whole.shape, whole.dtype),
        grid_spec=pltpu.PrefetchScalarGridSpec(
            num_scalar_prefetch=1,
            grid=(count,),
            in_specs=[pl.BlockSpec(memory_space=pl.ANY), pl.BlockSpec((1, *shape), lambda i, base: (i, 0, 0))],
            out_specs=pl.BlockSpec((1, *shape), lambda i, base: (base[0] + i, 0, 0)),
        ),
        input_output_aliases={1: 0},
        compiler_params=pltpu.CompilerParams(dimension_semantics=("arbitrary",), vmem_limit_bytes=16 * 1024 * 1024),
        cost_estimate=pl.CostEstimate(flops=8_000_000_000, bytes_accessed=30_000_000, transcendentals=0),
        name="merge",
    )(other_base, whole, other)


class Plan(NamedTuple):
    n_chunk: Any
    n_group: Any
    n_mix: Any
    seg_len: Any
    seg_src: Any
    seg_dst: Any
    seg_own: Any
    tail_at: Any
    tail_len: Any
    base: Any
    own_seq: Any
    rest_seq: Any
    dev_blocks: int = 0
    n_exp: int = 0


def exclusive(values, axis=0):
    return jnp.cumsum(values, axis=axis) - values


def make_plan(local_ids, own_blocks, n_exp, max_tiles, max_own, weight_base):
    onehot = (local_ids[:, :, None, :] == jnp.arange(n_exp)[None, None, :, None]).astype(jnp.float32)
    hits = jnp.sum(onehot, axis=1)
    before = jnp.triu(jnp.ones((BLOCK, BLOCK), jnp.bfloat16), 1)
    rank = jnp.einsum("oet,ts->oes", hits.astype(jnp.bfloat16), before, preferred_element_type=jnp.float32)
    seg_len = (jnp.sum(hits, axis=2).astype(jnp.int32) + GROUP - 1) // GROUP
    seg_src = exclusive(seg_len, 1)
    per_tile, per_half = TILE // GROUP, HALF // GROUP
    groups = jnp.stack([jnp.sum(seg_len[:own_blocks], axis=0), jnp.sum(seg_len[own_blocks:], axis=0)])
    both_tiles = (groups + per_tile - 1) // per_tile
    own_tiles, other_tiles = both_tiles
    tiles = own_tiles + other_tiles
    tile_base = exclusive(tiles)
    begins = jnp.stack([tile_base, tile_base + own_tiles]) * per_tile
    seg_dst = jnp.concatenate([begins[0] + exclusive(seg_len[:own_blocks], 0), begins[1] + exclusive(seg_len[own_blocks:], 0)])
    place = rank + (seg_src * GROUP).astype(jnp.float32)[:, :, None]
    pos = jnp.sum(onehot * (place[:, None] + 1.0), axis=2).astype(jnp.int32) - 1
    exp_ids = jnp.arange(n_exp)

    def sequence(counts, length):
        ids = jnp.arange(length)
        at = jnp.minimum(ids, jnp.maximum(jnp.sum(counts) - 1, 0))
        ends = jnp.cumsum(counts)
        exp = jnp.minimum(jnp.sum((at[:, None] >= ends[None, :]).astype(jnp.int32), axis=1), n_exp - 1)
        is_exp = (exp[:, None] == exp_ids[None, :]).astype(jnp.int32)
        pick = lambda table: jnp.sum(is_exp * table[None, :], axis=1)
        return exp, at - pick(ends - counts), ids > at, pick

    def kind_of(left, past):
        return jnp.where(past, 0, jnp.where(left <= per_half, 1, 2))

    o_exp, o_nth, o_past, o_pick = sequence(own_tiles, max_own)
    own_base = exclusive(own_tiles)

    def rest_seq(half):
        mine = exp_ids // (n_exp // 2) == half
        exp, nth, past, pick = sequence(jnp.where(mine, tiles, 0), max_tiles // 2)
        own_count = pick(own_tiles)
        is_own = nth < own_count
        kind = kind_of(jnp.where(is_own, pick(groups[0]) - nth * per_tile, pick(groups[1]) - (nth - own_count) * per_tile), past)
        seq = (
            exp,
            pick(tile_base) + nth,
            pick(own_base) + jnp.minimum(nth, own_count - 1),
            jnp.where(is_own, kind, 0),
            jnp.where(is_own, 0, kind),
            (nth == 0) & ~past,
            (nth == pick(tiles) - 1) & ~past,
        )
        return seq

    stack_rows = jnp.sum(seg_len, axis=1) * GROUP
    plan = Plan(
        n_chunk=(stack_rows + CHUNK - 1) // CHUNK,
        n_group=jnp.sum(seg_len, axis=1),
        n_mix=(stack_rows + MIX - 1) // MIX,
        seg_len=seg_len.reshape(-1),
        seg_src=seg_src.reshape(-1),
        seg_dst=seg_dst.reshape(-1),
        seg_own=(own_base[None, :] * per_tile + exclusive(seg_len, 0)).reshape(-1),
        tail_at=(begins + groups).reshape(-1),
        tail_len=((groups + per_half - 1) // per_half * per_half - groups).reshape(-1),
        base=weight_base.reshape(1),
        own_seq=(o_exp + weight_base, o_pick(tile_base) + o_nth, o_pick(own_base) + o_nth, kind_of(o_pick(groups[0]) - o_nth * per_tile, o_past)),
        rest_seq=(rest_seq(0), rest_seq(1)),
    )
    return jax.tree.map(lambda value: jnp.asarray(value, jnp.int32), plan), pos


def solution(mesh):
    ep_size = mesh.shape["ep"]
    dp_size = mesh.shape["dp"]
    devices = ep_size * dp_size
    cores = 2
    tok_spec = P(("dp", "ep"), None)
    exp_spec = P("ep", None, None)
    core_perm = [(i, i ^ 1) for i in range(dp_size)]
    x_perm = [(i, i ^ cores) for i in range(dp_size)]
    ep_perm = [(i, i ^ 1) for i in range(ep_size)]

    def to_core(away):
        return lax.ppermute(away, "dp", core_perm)

    def to_ep(far):
        return lax.ppermute(far, "ep", ep_perm)

    def to_x(block):
        return lax.ppermute(block, "dp", x_perm)

    def spread(block):
        ep_block = to_ep(block)
        core_block = to_core(block)
        own = (to_core(ep_block), core_block, ep_block, block)
        return own, (to_x(block), to_x(ep_block))

    def after(value, other):
        return lax.optimization_barrier((value, other))

    def device_step(tokens, d_out, expert_ids, norm_gain, router, w_gate, w_up, w_down):
        tok_rows, _ = tokens.shape
        top_k = expert_ids.shape[1]
        local_experts = w_gate.shape[0]
        experts = local_experts * ep_size
        total_tok = tok_rows * devices
        n_exp = local_experts // cores
        dev_blocks = tok_rows // BLOCK
        own_devs = devices // 2
        own_blocks = own_devs * dev_blocks
        max_own = n_exp * -(-(own_devs * MAX_HITS + own_blocks * (GROUP - 1)) // TILE)
        max_tiles = 2 * max_own

        ep_at = lax.axis_index("ep")
        dp_at = lax.axis_index("dp")
        core_at = lax.rem(dp_at, cores)
        x_at = lax.div(dp_at, cores)

        def dev_of(x, core, ep):
            return (x * cores + core) * ep_size + ep

        dev_order = jnp.stack(
            [dev_of(x_at, 1 - core_at, 1 - ep_at), dev_of(x_at, 1 - core_at, ep_at), dev_of(x_at, core_at, 1 - ep_at), dev_of(x_at, core_at, ep_at)]
            + [dev_of(1 - x_at, core_at, ep_at), dev_of(1 - x_at, core_at, 1 - ep_at), dev_of(1 - x_at, 1 - core_at, ep_at), dev_of(1 - x_at, 1 - core_at, 1 - ep_at)]
        )
        tokens32 = tokens.astype(jnp.float32)
        gain32 = norm_gain.astype(jnp.float32)
        inv_rms, normed = norm_forward(tokens32, gain32)
        logits = jnp.dot(normed, router, preferred_element_type=jnp.float32)
        router_probs = jax.nn.softmax(logits, axis=1)
        expert_hits = expert_ids[:, :, None] == jnp.arange(experts)[None, None, :]
        gate_vals = jnp.sum(jnp.where(expert_hits, router_probs[:, None, :], 0.0), axis=2)

        id_packets = lax.all_gather(expert_ids.astype(jnp.float32).T, ("dp", "ep"))
        d_out_late, id_packets = after(d_out, id_packets)
        own_d_out, x_d_out = spread(d_out_late)
        all_ids = id_packets.astype(jnp.int32)
        counts = jnp.sum((all_ids[..., None] == jnp.arange(experts)).astype(jnp.float32), axis=(0, 1, 2))
        expert_frac = counts / (total_tok * top_k)


        def by_block(rows):
            return rows.reshape(devices, top_k, dev_blocks, BLOCK).transpose(0, 2, 1, 3).reshape(devices * dev_blocks, top_k, BLOCK)

        first_expert = ep_at * local_experts + core_at * n_exp
        block_ids = by_block(jnp.take(id_packets, dev_order, axis=0)).astype(jnp.int32) - first_expert
        block_ids = jnp.where((block_ids >= 0) & (block_ids < n_exp), block_ids, n_exp)
        plan, pos = make_plan(block_ids, own_blocks, n_exp, max_tiles, max_own, core_at * n_exp)
        plan = plan._replace(dev_blocks=dev_blocks, n_exp=n_exp)
        prob_sums = jnp.pad(jnp.sum(router_probs, axis=0), (0, tok_rows - experts))
        packet, (pos, tail_at) = after(jnp.concatenate([gate_vals.T, prob_sums[None]], axis=0), (pos, plan.tail_at))
        plan = plan._replace(tail_at=tail_at)
        packets = lax.all_gather(packet, ("dp", "ep"))
        normed_late, packets = after(normed, packets)
        own_normed, x_normed = spread(normed_late)
        block_gates = by_block(jnp.take(packets, dev_order, axis=0)[:, :top_k])
        pos_t = pos[:own_blocks].transpose(0, 2, 1)
        gates_t = block_gates[:own_blocks].transpose(0, 2, 1)

        aux_loss = AUX_COEF * experts * jnp.sum(expert_frac * jnp.sum(packets[:, top_k, :experts], axis=0)) / total_tok
        rows = max_tiles * TILE
        d_rows = dispatch(own_d_out, pos, block_gates, plan, 0, None, rows, True)
        x = dispatch(own_normed, pos, block_gates, plan, 0, None, rows, False)
        hidden, d_act_gate, d_act_up, result, d_expert_in = own_tiles(x, d_rows, w_gate, w_up, w_down, plan)
        d_rows, result = after(d_rows, result)
        x_d_out, result = after(x_d_out, result)
        x_normed, result = after(x_normed, result)
        x_d_out = (*x_d_out, *(to_core(block) for block in x_d_out))
        x_normed = (*x_normed, *(to_core(block) for block in x_normed))
        half, quarter = own_blocks // 2, own_blocks // 4
        d_away, d_far, d_near = combine(d_expert_in, pos_t, gates_t, None, plan, 0, (half, quarter, quarter), False)
        result, d_away = after(result, d_away)
        d_met = to_core(d_away)
        away, d_gate_away = combine(result, pos_t, gates_t, own_d_out[:2], plan, 0, (half,), True)
        result, (away, d_gate_away, d_far) = after(result, (away, d_gate_away, d_far + d_met[:tok_rows]))
        d_crossed = to_ep(d_far)
        met = to_core(away)
        d_gate_met = to_core(d_gate_away)
        far, near, d_gate_mine = combine(result, pos_t, gates_t, own_d_out[2:], plan, half, (quarter, quarter), True)
        d_gate_mine = d_gate_mine + d_gate_met
        hidden, (far, d_gate_far) = after(hidden, (far + met[:tok_rows], d_gate_mine[:quarter]))
        crossed = to_ep(far)
        d_gate_crossed = to_ep(d_gate_far)
        d_rows, hidden = after(d_rows, hidden)
        d_rows = dispatch(x_d_out, pos, block_gates, plan, own_blocks, d_rows, rows, True)
        x = dispatch(x_normed, pos, block_gates, plan, own_blocks, x, rows, False)
        grads, wholes = [None, None], None
        for part in range(2):
            *grads[part], all_gate, all_up, all_down = rest_tiles(x, d_rows, w_gate, w_up, w_down, hidden, d_act_gate, d_act_up, plan, part, wholes)
            wholes = (all_gate, all_up, all_down)
        d_gates = (d_gate_mine[quarter:] + d_gate_crossed).reshape(tok_rows, top_k)
        d_probs = jnp.sum(jnp.where(expert_hits, d_gates[:, :, None], 0.0), axis=1) + (AUX_COEF * experts / total_tok) * expert_frac[None, :]
        d_logits = (router_probs * (d_probs - jnp.sum(router_probs * d_probs, axis=1, keepdims=True))).astype(jnp.bfloat16)
        grad_router = lax.psum(lax.dot_general(normed, d_logits, TN_DIMS, preferred_element_type=jnp.float32), ("ep", "dp"))
        other_base = (1 - core_at).reshape(1).astype(jnp.int32) * n_exp
        wholes = list(wholes)
        for part in range(2):
            for i in range(3):
                wholes[i] = merge(wholes[i], to_core(grads[part][i]), other_base + part * (n_exp // 2))
        all_gate, all_up, all_down = wholes
        layer_out = (tokens32 + (near + met[tok_rows:] + crossed)).astype(jnp.bfloat16)
        d_normed = (d_near + d_met[tok_rows:] + d_crossed) + lax.dot_general(d_logits, router, NT_DIMS, preferred_element_type=jnp.float32)
        d_tokens = (d_out.astype(jnp.float32) + norm_backward(tokens32, inv_rms, gain32, d_normed)).astype(jnp.bfloat16)
        return layer_out, aux_loss.reshape(1), d_tokens, grad_router, all_gate, all_up, all_down

    return jax.shard_map(device_step, mesh=mesh, in_specs=(tok_spec, tok_spec, tok_spec, P(None), P(None, None), exp_spec, exp_spec, exp_spec), out_specs=(tok_spec, P(None), tok_spec, P(None, None), exp_spec, exp_spec, exp_spec), check_vma=False)
```
